1024 devices in a mesh: group: 2 (over core), row: 8 (over z_lo), col: 64 (over x, y, z_hi).
Axes of the slice: x: 4, y: 4, z: 32 (z_hi: 4, z_lo: 8; z = z_hi * 8 + z_lo), core: 2. Of those that a mesh axis runs over, the one named last changes fastest.
Arguments:
- velocity_hat: float32 [3, 2, 16, 512, 512], P(None, None, ('group', 'row'), 'col'), may hold values from -6 to 6
- scalar: float32 [16, 1024, 1024], P('group', 'col', 'row'), may hold values from -6 to 6
- tile_offset: int32 [1], replicated, may hold values from 0 to 511
Outputs:
- velocity_new: float32 [3, 2, 16, 512, 512], P(None, None, ('group', 'row'), 'col')
- scalar_new: float32 [16, 1024, 1024], P('group', 'col', 'row')
The draws below stay inside these ranges and needn't reach their ends.
Inputs may be any that keep to these rules, and one draw needn't show every extreme that they name: `tile_offset`: one offset for every tile and plane.
All inputs are finite; a program needn't handle non-finite values.
Results may differ from the reference program's by a relative error of at most 0.000076.
Values sent between devices are 32-bit elements; how exact they have to be, the bound alone decides.
A program may use at most 32 MiB of HBM per device.

```python
import jax
import jax.numpy as jnp
from jax import lax

GRID = 512
PLANES = 16
FINE = 1024


def shard_levels(key, shape, pieces, least, high):
    factor_of, own = 1.0, jax.random.fold_in(key, 6)
    for axis_at, blocks in pieces:
        steps = jnp.exp(jax.random.uniform(jax.random.fold_in(own, axis_at), (blocks,), jnp.float32, least / len(pieces), high / len(pieces)))
        factor_of = factor_of * jnp.repeat(steps, shape[axis_at] // blocks).reshape([-1 if axis == axis_at else 1 for axis in range(len(shape))])
    return factor_of


def centred(own_key, shape, scale, reach, pieces=(), kind=jnp.bfloat16):
    loudness = shard_levels(own_key, shape, pieces, -0.22, 0.18) if pieces else 1.0
    array = jax.random.normal(own_key, shape, jnp.float32) * scale * loudness
    return jnp.minimum(jnp.maximum(array, -reach), reach).astype(kind)


def setup_inputs(seed: int = 0) -> dict:
    key_of = jax.random.split(jax.random.key(seed), 4)
    velocity_hat = centred(key_of[0], (3, 2, PLANES, GRID, GRID), 1.0, 6.0, ((2, 16), (3, 64)), jnp.float32)
    scalar = centred(key_of[1], (PLANES, FINE, FINE), 1.0, 6.0, ((0, 2), (1, 64), (2, 8)), jnp.float32)
    tile_offset = jax.random.randint(key_of[2], (1,), 0, GRID).astype(jnp.int32)
    return dict(velocity_hat=velocity_hat, scalar=scalar, tile_offset=tile_offset)


time_step = 0.25
viscosity = 2.0
diffusivity = 0.15
substep = 0.2


def signed(length):
    indices = jnp.arange(length, dtype=jnp.int32)
    return jnp.where(indices < length // 2, indices, indices - length)


def plane_step(plane):
    extent = plane.shape[-1]
    wavenumber = signed(extent)
    scaled = wavenumber.astype(jnp.float32) / (extent // 2)
    kappa_x = scaled[:, None]
    kappa_y = scaled[None, :]
    spectra = plane[:, 0] + 1j * plane[:, 1]
    spin_x = 1j * kappa_y * spectra[2]
    spin_y = -1j * kappa_x * spectra[2]
    spin_z = 1j * kappa_x * spectra[1] - 1j * kappa_y * spectra[0]
    combined = jnp.concatenate([spectra, jnp.stack([spin_x, spin_y, spin_z])])
    physical = jnp.fft.ifft2(combined, axes=(-2, -1), norm="ortho").real
    x_speed, y_speed, z_speed, omega_x, omega_y, omega_z = [physical[n] for n in range(6)]
    product = jnp.stack([y_speed * omega_z - z_speed * omega_y,
                         z_speed * omega_x - x_speed * omega_z,
                         x_speed * omega_y - y_speed * omega_x])
    forcing = jnp.fft.fft2(product, axes=(-2, -1), norm="ortho")
    retained = (3 * jnp.abs(wavenumber)[:, None] < extent) & (3 * jnp.abs(wavenumber)[None, :] < extent)
    damping = jnp.exp(-viscosity * time_step * (kappa_x ** 2 + kappa_y ** 2))
    updated = damping * (spectra + time_step * jnp.where(retained, forcing, 0.0))
    velocity = jnp.stack([updated.real, updated.imag], axis=1).astype(jnp.float32)
    return velocity, jnp.swapaxes(physical[:2], -1, -2).astype(jnp.float32)


def advance(values, x_speed, y_speed):
    def neighbor(step_y, step_x):
        return jnp.roll(values, (-step_y, -step_x), axis=(1, 2))
    grad_x = (neighbor(0, -2) - neighbor(0, 2) + 8.0 * (neighbor(0, 1) - neighbor(0, -1))) / 12.0
    grad_y = (neighbor(-2, 0) - neighbor(2, 0) + 8.0 * (neighbor(1, 0) - neighbor(-1, 0))) / 12.0
    lap_x = (16.0 * (neighbor(0, 1) + neighbor(0, -1)) - neighbor(0, 2) - neighbor(0, -2) - 30.0 * values) / 12.0
    lap_y = (16.0 * (neighbor(1, 0) + neighbor(-1, 0)) - neighbor(2, 0) - neighbor(-2, 0) - 30.0 * values) / 12.0
    return values + substep * (diffusivity * (lap_x + lap_y) - (x_speed * grad_x + y_speed * grad_y))


def reference(velocity_hat, scalar, tile_offset):
    extent = velocity_hat.shape[-1]
    planes_first = jnp.moveaxis(velocity_hat, 2, 0)
    velocity_planes, speed_planes = lax.map(plane_step, planes_first)
    velocity_new = jnp.moveaxis(velocity_planes, 0, 2)
    horizontal = jnp.moveaxis(speed_planes, 0, 1)
    count = horizontal.shape[1]
    shifted = jnp.roll(horizontal, -tile_offset[0], axis=3)
    following = jnp.roll(shifted, -1, axis=3)
    refined_x = jnp.stack([shifted, (shifted + following) * 0.5], axis=4).reshape(2, count, extent, 2 * extent)
    following_y = jnp.roll(refined_x, -1, axis=2)
    refined = jnp.stack([refined_x, (refined_x + following_y) * 0.5], axis=3).reshape(2, count, 2 * extent, 2 * extent)
    halfway = advance(scalar, refined[0], refined[1])
    scalar_new = advance(halfway, refined[0], refined[1])
    return velocity_new, scalar_new
```

```python
import math

import jax
import jax.numpy as jnp
import numpy as np
from jax import lax
from jax.experimental import pallas as pl
from jax.experimental.pallas import tpu as pltpu
from jax.sharding import PartitionSpec as P

time_step = 0.25
viscosity = 2.0
diffusivity = 0.15
substep = 0.2
MESH = pl.DeviceIdType.MESH

N, NC, NL = 512, 64, 8
KEPT = [0, 1, 2, 3, 4, 5, 10, 11, 12, 13, 14, 15]
ORDER = KEPT + [6, 7, 8, 9]


def tables():
    unit = 1.0 / math.sqrt(N)
    wave = np.arange(N)
    wave = np.where(wave < N // 2, wave, wave - N) / (N // 2)
    eye = np.eye(8)
    c_natural = np.arange(64)
    c_zw = np.array([4 * w + z for z in range(4) for w in range(16)])
    c_kept = np.array([4 * w + z for z in range(4) for w in ORDER])
    rows = np.arange(64)

    def angle(left, right, length):
        return 2 * np.pi * ((left[:, None] * right[None, :]) % length) / length

    eighth = np.arange(8)
    turn = np.exp(1j * angle(eighth, eighth, 8)) * unit

    first = []
    for e in range(2):
        part = np.zeros((2, 4, 8, 2, 2, 8, 8))
        for m in range(4):
            for l in range(8):
                v = turn[2 * m + e, l]
                for j in range(8):
                    part[0, m, j, 0, 0, l, j] = v.real
                    part[1, m, j, 0, 0, l, j] = -v.imag
                    part[0, m, j, 0, 1, l, j] = v.imag
                    part[1, m, j, 0, 1, l, j] = v.real
        part[:, :, :, 1, 0] = -part[:, :, :, 0, 1]
        part[:, :, :, 1, 1] = part[:, :, :, 0, 0]
        first.append(part.reshape(64, 256))

    lane = np.arange(128)
    twist_y = angle(rows, (lane // 8) % 8, N)
    twist_x = angle(rows, lane % 8, N)

    mixed = np.zeros((2, 2, 8, 8, 2, 8, 8))
    forward = np.zeros((2, 8, 8, 2, 2, 8, 8))
    last = [np.zeros((2, 2, 8, 8, 2, 4, 8)) for _ in range(2)]
    for l in range(8):
        for j in range(8):
            for p in range(8):
                v = turn[j, p]
                for half in range(2):
                    mixed[0, 0, l, j, half, p, l] = v.real
                    mixed[0, 1, l, j, half, p, l] = -v.imag
                    mixed[1, 0, l, j, half, p, l] = -v.imag
                    mixed[1, 1, l, j, half, p, l] = -v.real
                forward[0, p, l, 0, 0, l, j] = v.real
                forward[0, p, l, 0, 1, l, j] = -v.imag
                forward[0, p, l, 1, 0, l, j] = v.imag
                forward[0, p, l, 1, 1, l, j] = v.real
            for m in range(4):
                for e in range(2):
                    v = turn[2 * m + e, l]
                    t = last[e]
                    t[0, 0, l, j, 0, m, j] = v.real
                    t[1, 1, l, j, 0, m, j] = v.real
                    t[0, 1, l, j, 0, m, j] = v.imag
                    t[1, 0, l, j, 0, m, j] = -v.imag
                    t[0, 1, l, j, 1, m, j] = v.real
                    t[1, 0, l, j, 1, m, j] = -v.real
                    t[0, 0, l, j, 1, m, j] = -v.imag
                    t[1, 1, l, j, 1, m, j] = -v.imag
    forward_y = np.zeros_like(forward)
    forward_y[1] = forward[0]

    def pair(order):
        t = angle(order, rows, 64)
        return np.concatenate([np.cos(t), np.sin(t)], axis=1)

    stacked = angle(rows, c_zw, 64)
    kappa_y = np.zeros((2, 64, 2, 4, 8))
    for e in range(2):
        for m in range(4):
            kappa_y[e, :, :, m, :] = wave[64 * (2 * m + e) + rows][:, None, None]
    kappa_x = wave[8 * c_zw[:, None] + (lane % 8)[None, :]]

    spread = np.zeros((128, 256))
    for f in range(-2, 130):
        k = f // 2 + 1
        if f % 2 == 0:
            spread[k, f % 256] = 1.0
        else:
            spread[k, f % 256] = 0.5
            spread[k + 1, f % 256] = 0.5
    lift = np.zeros((2, 24, 24))
    for v in range(2):
        def slot(row):
            if row < 0:
                return 20 + v
            return 8 * v + row if row < 8 else 16 + 2 * v + row - 8
        for f in range(-2, 18):
            k = f // 2
            if f % 2 == 0:
                lift[v, f + 4, slot(k)] = 1.0
            else:
                lift[v, f + 4, slot(k)] = 0.5
                lift[v, f + 4, slot(k + 1)] = 0.5

    out = dict(
        first0=first[0], first1=first[1],
        tyc=np.cos(twist_y), tys=np.sin(twist_y), txc=np.cos(twist_x), txs=np.sin(twist_x),
        cs1=pair(c_natural), cs3=np.concatenate([np.cos(stacked).T, np.sin(stacked).T]).reshape(2, 64, 64).transpose(0, 1, 2).reshape(128, 64),
        mixed=mixed.reshape(256, 128), fx=forward.reshape(128, 256), fy=forward_y.reshape(128, 256),
        cs4=pair(c_kept), last0=last[0].reshape(256, 64), last1=last[1].reshape(256, 64),
        ky=kappa_y.reshape(128, 64), kx=kappa_x, spread=spread, lift=lift.reshape(48, 24),
    )
    flat = angle(rows, c_zw, 64)
    out["cs3"] = np.concatenate([np.cos(flat), np.sin(flat)], axis=0)
    return {k: np.asarray(v, np.float32) for k, v in out.items()}


NAMES = ["first0", "first1", "tyc", "tys", "txc", "txs", "cs1", "cs3", "mixed", "fx", "fy", "cs4",
         "last0", "last1", "ky", "kx", "spread", "lift"]


def dot(a, b):
    return jnp.dot(a, b, precision=lax.Precision.HIGHEST, preferred_element_type=jnp.float32)


def inverse_y(t, spectra, kappa_x):
    turned = []
    for comp in range(3):
        stacked = jnp.concatenate(
            [spectra(comp, ri)[:, 128 * m : 128 * m + 128] for ri in range(2) for m in range(4)], axis=0
        )
        turned.append(stacked.T)
    spin_x = turned[2] * t["ky"]
    spin_z = turned[1] * kappa_x - turned[0] * t["ky"]
    fields = turned + [spin_x, spin_z]
    even = jnp.concatenate([f[:64] for f in fields], axis=0)
    odd = jnp.concatenate([f[64:] for f in fields], axis=0)
    mixed = dot(even, t["first0"]) + dot(odd, t["first1"])
    upper, lower = [], []
    for n in range(5):
        plain = mixed[64 * n : 64 * n + 64, :128]
        times_i = mixed[64 * n : 64 * n + 64, 128:]
        if n >= 3:
            plain, times_i = times_i, -plain
        upper.append(plain * t["tyc"] + times_i * t["tys"])
        lower.append(times_i * t["tyc"] - plain * t["tys"])
    both = jnp.concatenate([jnp.concatenate(upper, axis=1), jnp.concatenate(lower, axis=1)], axis=0)
    blocks = dot(t["cs1"], both)
    return [blocks[:, 128 * n : 128 * n + 128] for n in range(5)]


def inverse_x(t, blocks):
    u, v, w, spin_x, spin_z = blocks
    six = [u, v, w, spin_x, w * t["kx"], spin_z]
    summed = dot(t["cs3"], jnp.concatenate(six, axis=1))
    rows = []
    for n in range(6):
        first = summed[:64, 128 * n : 128 * n + 128]
        second = summed[64:, 128 * n : 128 * n + 128]
        a = first * t["txc"] - second * t["txs"]
        b = first * t["txs"] + second * t["txc"]
        if n == 4:
            a, b = b, -a
        rows.append(jnp.concatenate([a, b], axis=1))
    fields = dot(jnp.concatenate(rows, axis=0), t["mixed"])
    return [fields[64 * n : 64 * n + 64] for n in range(6)]


def forward_x(t, fields):
    u, v, w, ox, oy, oz = fields
    left = lax.broadcasted_iota(jnp.int32, (64, 128), 1) < 64
    product_xy = jnp.where(left, v, w) * jnp.where(left, oz, ox) - jnp.where(left, w, u) * jnp.where(left, oy, oz)
    product_z = u * oy - v * ox
    mixed = [dot(product_xy, t["fx"]), dot(product_xy, t["fy"]), dot(product_z, t["fx"])]
    upper, lower = [], []
    for m in mixed:
        plain, times_i = m[:, :128], m[:, 128:]
        upper.append(plain * t["txc"] - times_i * t["txs"])
        lower.append(-(times_i * t["txc"] + plain * t["txs"]))
    both = jnp.concatenate([jnp.concatenate(upper, axis=1), jnp.concatenate(lower, axis=1)], axis=0)
    blocks = dot(t["cs4"], both)
    return [blocks[:, 128 * n : 128 * n + 128] for n in range(3)]


def forward_y(t, blocks):
    summed = dot(t["cs3"], jnp.concatenate(blocks, axis=1))
    rows = []
    for n in range(3):
        first = summed[:64, 128 * n : 128 * n + 128]
        second = summed[64:, 128 * n : 128 * n + 128]
        rows.append(
            jnp.concatenate(
                [first * t["tyc"] - second * t["tys"], first * t["tys"] + second * t["tyc"]], axis=1
            )
        )
    rows = jnp.concatenate(rows, axis=0)
    even, odd = dot(rows, t["last0"]), dot(rows, t["last1"])
    return [
        jnp.concatenate([even[64 * n : 64 * n + 64], odd[64 * n : 64 * n + 64]], axis=0).T for n in range(3)
    ]


def kernel(vh, sc, off, *rest):
    t = {name: rest[i] for i, name in enumerate(NAMES)}
    (vnew, snew, send1, recv1, send2, recv2, relay2, send3, recv3, relay3a, relay3b, send4, recv4,
     vsend, vrecv, vlo_s, vhi_s, vlo_r, vhi_r, sx, sy_s, sy_r, tile, side, coarse, fine,
     s1, r1, s2, r2, s3, r3, s4, r4, sv, rv, sm, rm) = rest[len(NAMES):]
    t = {name: ref[...] for name, ref in t.items()}

    g = lax.axis_index("group")
    r = lax.axis_index("row")
    c = lax.axis_index("col")
    w, z = c // 4, c % 4
    z_up, z_down, z_far = (z + 1) % 4, (z + 3) % 4, (z + 2) % 4
    up, down = (g, r, 4 * w + z_up), (g, r, 4 * w + z_down)
    c_next, c_prev = (g, r, (c + 1) % 64), (g, r, (c + 63) % 64)
    r_next, r_prev = (g, (r + 1) % 8, c), (g, (r + 7) % 8, c)
    plane_peers = [(g, r, 4 * ((w + d) % 16) + z) for d in range(1, 16)]
    row_peers = [(g, (r + d) % 8, c) for d in range(1, 8)]
    kept = jnp.logical_or(w < 6, w >= 10)

    barrier = pltpu.get_barrier_semaphore()
    greeted = plane_peers + row_peers + [up, down, c_next, c_prev]
    for peer in greeted:
        pl.semaphore_signal(barrier, inc=1, device_id=peer, device_id_type=MESH)

    def remote(src, dst, ssem, rsem, peer):
        return pltpu.make_async_remote_copy(
            src_ref=src, dst_ref=dst, send_sem=ssem, recv_sem=rsem, device_id=peer, device_id_type=MESH
        )

    def rows(ref, start, size):
        return ref.at[pl.ds(pl.multiple_of(start, 8), size), :]

    lane64 = lax.broadcasted_iota(jnp.int32, (1, 64), 1)
    wave = 8 * c + lane64 % 8
    kappa = jnp.where(wave < 256, wave, wave - 512).astype(jnp.float32) * (1.0 / 256.0)
    blocks = inverse_y(t, lambda comp, ri: vh[2 * comp + ri], kappa)
    zero = jnp.zeros((4, 128), jnp.float32)
    for d in range(16):
        part = [b[4 * d : 4 * d + 4] for b in blocks] + [zero]
        send1[24 * d : 24 * d + 24, :] = jnp.concatenate(part, axis=0)

    side[...] = jnp.zeros_like(side)
    coarse[...] = jnp.zeros_like(coarse)

    pl.semaphore_wait(barrier, len(greeted))

    sent1 = []
    for d in range(1, 16):
        to = (w + d) % 16
        copy = remote(rows(send1, 24 * to, 24), rows(recv1, 24 * w, 24), s1.at[d], r1.at[d], plane_peers[d - 1])
        copy.start()
        sent1.append(copy)
    tile_right = remote(sc, sx.at[0], sm.at[0], rm.at[0], r_next)
    tile_left = remote(sc, sx.at[1], sm.at[1], rm.at[1], r_prev)
    tile_right.start()
    tile_left.start()
    mine = pl.ds(pl.multiple_of(24 * w, 8), 24)
    recv1[mine, :] = send1[mine, :]
    for copy in sent1:
        copy.wait_recv()
    for k in range(4):
        for f in range(5):
            send2[k, 16 * f : 16 * f + 16, :] = recv1[pl.ds(4 * f + k, 16, stride=24), :]

    half = 40
    far_up = remote(send2.at[z_far, pl.ds(0, half)], relay2.at[0], s2.at[0], r2.at[0], up)
    far_down = remote(send2.at[z_far, pl.ds(half, half)], relay2.at[1], s2.at[1], r2.at[1], down)
    near_up = remote(send2.at[z_up], recv2.at[z], s2.at[2], r2.at[2], up)
    near_down = remote(send2.at[z_down], recv2.at[z], s2.at[3], r2.at[3], down)
    far_up.start()
    far_down.start()
    near_up.start()
    near_down.start()
    recv2[z] = send2[z]
    far_up.wait_recv()
    pass_up = remote(relay2.at[0], recv2.at[z_down, pl.ds(0, half)], s2.at[4], r2.at[4], up)
    pass_up.start()
    far_down.wait_recv()
    pass_down = remote(relay2.at[1], recv2.at[z_up, pl.ds(half, half)], s2.at[5], r2.at[5], down)
    pass_down.start()

    tile_right.wait_recv()
    tile_left.wait_recv()
    first_half = lax.broadcasted_iota(jnp.int32, (16, 128), 1) < 64
    for p in range(8):
        tile[24 * p + 4 : 24 * p + 20, :] = sc[p]
        side[24 * p + 4 : 24 * p + 20, :] = jnp.where(first_half, sx[1, p], sx[0, p])
    for i in range(4):
        sy_s[0, 8 * i : 8 * i + 8, :] = tile[pl.ds(16 + i, 8, stride=24), :]
        sy_s[1, 8 * i : 8 * i + 8, :] = tile[pl.ds(4 + i, 8, stride=24), :]
    for i in range(2):
        sy_s[0, 32 + 8 * i : 40 + 8 * i, :] = side[pl.ds(18 + i, 8, stride=24), :]
        sy_s[1, 32 + 8 * i : 40 + 8 * i, :] = side[pl.ds(4 + i, 8, stride=24), :]
    rim_next = remote(sy_s.at[0], sy_r.at[0], sm.at[2], rm.at[2], c_next)
    rim_prev = remote(sy_s.at[1], sy_r.at[1], sm.at[3], rm.at[3], c_prev)
    rim_next.start()
    rim_prev.start()

    near_up.wait_recv()
    near_down.wait_recv()
    pass_up.wait_recv()
    pass_down.wait_recv()

    landed = [
        jnp.concatenate([recv2[k, 16 * f : 16 * f + 16, :] for k in range(4)], axis=0) for f in range(5)
    ]
    fields = inverse_x(t, landed)
    leaving = forward_x(t, fields)
    for k in range(4):
        for f in range(3):
            send3[k, 12 * f : 12 * f + 12, :] = leaving[f][16 * k : 16 * k + 12]
        send3[k, 36:40, :] = zero
    far_up3 = remote(send3.at[z_far, pl.ds(0, 24)], relay3a, s3.at[0], r3.at[0], up)
    far_down3 = remote(send3.at[z_far, pl.ds(24, 16)], relay3b, s3.at[1], r3.at[1], down)
    near_up3 = remote(send3.at[z_up], rows(recv3, 40 * z, 40), s3.at[2], r3.at[2], up)
    near_down3 = remote(send3.at[z_down], rows(recv3, 40 * z, 40), s3.at[3], r3.at[3], down)
    far_up3.start()
    far_down3.start()
    near_up3.start()
    near_down3.start()
    recv3[pl.ds(pl.multiple_of(40 * z, 8), 40), :] = send3[z]

    left = lax.broadcasted_iota(jnp.int32, (64, 128), 1) < 64
    speeds = jnp.where(left, fields[0], fields[1]).T
    lines = []
    for f in range(2):
        lines.append(
            jnp.concatenate([speeds[64 * f + 8 * p : 64 * f + 8 * p + 8, :] for p in range(8)], axis=1)
        )
    lines = jnp.concatenate(lines, axis=0)
    rolled = pltpu.roll(lines, (513 - off[0]) % 512, 1)
    shifted = pltpu.roll(rolled, 448, 1)
    for k in range(4):
        vsend[2 * k] = rolled[:, 128 * k : 128 * k + 128]
        vsend[2 * k + 1] = shifted[:, 128 * k : 128 * k + 128]
    sentv = []
    for d in range(1, 8):
        copy = remote(vsend.at[(r + d) % 8], rows(vrecv, 16 * r, 16), sv.at[d], rv.at[d], row_peers[d - 1])
        copy.start()
        sentv.append(copy)
    vrecv[pl.ds(pl.multiple_of(16 * r, 8), 16), :] = vsend[r]

    far_up3.wait_recv()
    pass_up3 = remote(relay3a, rows(recv3, 40 * z_down, 24), s3.at[4], r3.at[4], up)
    pass_up3.start()
    far_down3.wait_recv()
    pass_down3 = remote(relay3b, rows(recv3, 40 * z_up + 24, 16), s3.at[5], r3.at[5], down)
    pass_down3.start()

    for copy in sentv:
        copy.wait_recv()
    for i, k in enumerate((0, 1, 8, 9)):
        vlo_s[8 * i : 8 * i + 8, :] = vrecv[pl.ds(k, 8, stride=16), :]
    for i, k in enumerate((7, 15)):
        vhi_s[8 * i : 8 * i + 8, :] = vrecv[pl.ds(k, 8, stride=16), :]
    low = remote(vlo_s, vlo_r, sm.at[4], rm.at[4], c_prev)
    high = remote(vhi_s, vhi_r, sm.at[5], rm.at[5], c_next)
    low.start()
    high.start()

    near_up3.wait_recv()
    near_down3.wait_recv()
    pass_up3.wait_recv()
    pass_down3.wait_recv()

    for k in range(12):
        part = [recv3[pl.ds(12 * f + k, 4, stride=40), :] for f in range(3)] + [zero]
        send4[k] = jnp.concatenate(part, axis=0)
    for d in range(1, 16):
        to = (w + d) % 16
        slot = jnp.where(to < 6, to, to - 4)

        @pl.when(jnp.logical_or(to < 6, to >= 10))
        def _():
            remote(send4.at[slot], rows(recv4, 16 * w, 16), s4.at[d], r4.at[d], plane_peers[d - 1]).start()

    @pl.when(kept)
    def _():
        recv4[pl.ds(pl.multiple_of(16 * w, 8), 16), :] = send4[jnp.where(w < 6, w, w - 4)]

    rim_next.wait_recv()
    rim_prev.wait_recv()
    for i in range(4):
        tile[pl.ds(i, 8, stride=24), :] = sy_r[0, 8 * i : 8 * i + 8, :]
        tile[pl.ds(20 + i, 8, stride=24), :] = sy_r[1, 8 * i : 8 * i + 8, :]
    for i in range(2):
        side[pl.ds(2 + i, 8, stride=24), :] = sy_r[0, 32 + 8 * i : 40 + 8 * i, :]
        side[pl.ds(20 + i, 8, stride=24), :] = sy_r[1, 32 + 8 * i : 40 + 8 * i, :]
    for p in range(8):
        coarse[24 * p : 24 * p + 16, :] = vrecv[16 * p : 16 * p + 16, :]
    low.wait_recv()
    high.wait_recv()
    for i in range(4):
        coarse[pl.ds(16 + i, 8, stride=24), :] = vlo_r[8 * i : 8 * i + 8, :]
    for i in range(2):
        coarse[pl.ds(20 + i, 8, stride=24), :] = vhi_r[8 * i : 8 * i + 8, :]
    fine[...] = dot(coarse[...], t["spread"])

    def one_plane(p, carry):
        block = pl.ds(pl.multiple_of(24 * p, 8), 24)
        speed = dot(t["lift"], fine[block, :])
        x_speed, y_speed = speed[:24], speed[24:]
        values = jnp.concatenate([tile[block, :], side[block, :]], axis=1)
        for _ in range(2):
            values = advance(values, x_speed, y_speed)
        snew[p] = values[4:20, :128]
        return carry

    lax.fori_loop(0, 8, one_plane, 0)

    row8 = 8 * c + lax.broadcasted_iota(jnp.int32, (8, 128), 0)
    wave_x = jnp.where(row8 < 256, row8, row8 - 512)
    squared_x = jnp.square(wave_x.astype(jnp.float32) * (1.0 / 256.0))
    damping, keep = [], []
    for m in range(4):
        column = 128 * m + lax.broadcasted_iota(jnp.int32, (8, 128), 1)
        wave_y = jnp.where(column < 256, column, column - 512)
        squared_y = jnp.square(wave_y.astype(jnp.float32) * (1.0 / 256.0))
        damping.append(jnp.exp(-viscosity * time_step * (squared_x + squared_y)))
        keep.append(jnp.logical_and(3 * jnp.abs(wave_x) < 512, 3 * jnp.abs(wave_y) < 512))

    @pl.when(jnp.logical_not(kept))
    def _():
        for n in range(6):
            for m in range(4):
                lanes = slice(128 * m, 128 * m + 128)
                vnew[n, :, lanes] = damping[m] * vh[n, :, lanes]

    @pl.when(kept)
    def _():
        for d in range(1, 16):
            remote(send4.at[0], rows(recv4, 0, 16), s4.at[d], r4.at[d], plane_peers[d - 1]).wait_recv()
        gathered = [
            jnp.concatenate([recv4[pl.ds(4 * f + k, 16, stride=16), :] for k in range(4)], axis=0)
            for f in range(3)
        ]
        forcing = forward_y(t, gathered)
        for f in range(3):
            for ri in range(2):
                for m in range(4):
                    lanes = slice(128 * m, 128 * m + 128)
                    push = forcing[f][32 * ri + 8 * m : 32 * ri + 8 * m + 8]
                    n = 2 * f + ri
                    vnew[n, :, lanes] = damping[m] * (
                        vh[n, :, lanes] + time_step * jnp.where(keep[m], push, 0.0)
                    )

    for copy in sent1 + sentv + [
        tile_right, tile_left, far_up, far_down, near_up, near_down, pass_up, pass_down, rim_next, rim_prev,
        far_up3, far_down3, near_up3, near_down3, pass_up3, pass_down3, low, high,
    ]:
        copy.wait_send()
    for d in range(1, 16):
        to = (w + d) % 16

        @pl.when(jnp.logical_or(to < 6, to >= 10))
        def _():
            remote(send4.at[0], rows(recv4, 0, 16), s4.at[d], r4.at[d], plane_peers[d - 1]).wait_send()


def advance(values, x_speed, y_speed):
    height, breadth = values.shape

    def along(axis, step):
        return pltpu.roll(values, (-step) % values.shape[axis], axis)

    def parts(axis):
        two_back, back, ahead, two_ahead = (along(axis, s) for s in (-2, -1, 1, 2))
        grad = (two_back - two_ahead + 8.0 * (ahead - back)) * (1.0 / 12.0)
        lap = (16.0 * (ahead + back) - two_ahead - two_back - 30.0 * values) * (1.0 / 12.0)
        return grad, lap

    grad_x, lap_x = parts(1)
    grad_y, lap_y = parts(0)
    return values + substep * (diffusivity * (lap_x + lap_y) - (x_speed * grad_x + y_speed * grad_y))


def per_device(velocity_hat, scalar, tile_offset):
    consts = tables()
    f32 = jnp.float32
    vmem = pl.BlockSpec(memory_space=pltpu.VMEM)
    dma = pltpu.SemaphoreType.DMA

    def buf(*shape):
        return pltpu.VMEM(shape, f32)

    vnew, snew = pl.pallas_call(
        kernel,
        name="coupled_step",
        out_shape=(jax.ShapeDtypeStruct((6, 8, 512), f32), jax.ShapeDtypeStruct((8, 16, 128), f32)),
        in_specs=[vmem, vmem, pl.BlockSpec(memory_space=pltpu.SMEM)] + [vmem] * len(NAMES),
        out_specs=(vmem, vmem),
        scratch_shapes=[
            buf(384, 128), buf(384, 128), buf(4, 80, 128), buf(4, 80, 128), buf(2, 40, 128),
            buf(4, 40, 128), buf(160, 128), buf(24, 128), buf(16, 128), buf(12, 16, 128), buf(256, 128),
            buf(8, 16, 128), buf(128, 128), buf(32, 128), buf(16, 128), buf(32, 128), buf(16, 128),
            buf(2, 8, 16, 128), buf(2, 48, 128), buf(2, 48, 128), buf(192, 128), buf(192, 128),
            buf(192, 128), buf(192, 256),
            dma((16,)), dma((16,)), dma((6,)), dma((6,)), dma((6,)), dma((6,)), dma((16,)), dma((16,)),
            dma((8,)), dma((8,)), dma((6,)), dma((6,)),
        ],
        compiler_params=pltpu.CompilerParams(collective_id=0, has_side_effects=True),
    )(velocity_hat.reshape(6, 8, 512), scalar, tile_offset, *[jnp.asarray(consts[k]) for k in NAMES])
    return vnew.reshape(3, 2, 1, 8, 512), snew


def solution(mesh):
    return jax.shard_map(
        per_device,
        mesh=mesh,
        in_specs=(P(None, None, ("group", "row"), "col", None), P("group", "col", "row"), P()),
        out_specs=(P(None, None, ("group", "row"), "col", None), P("group", "col", "row")),
        check_vma=False,
    )
```

```python
import math

import jax
import jax.numpy as jnp
import numpy as np
from jax import lax
from jax.experimental import pallas as pl
from jax.experimental.pallas import tpu as pltpu
from jax.sharding import PartitionSpec as P

time_step = 0.25
viscosity = 2.0
diffusivity = 0.15
substep = 0.2
MESH = pl.DeviceIdType.MESH

N, NC, NL = 512, 64, 8
KEPT = [0, 1, 2, 3, 4, 5, 10, 11, 12, 13, 14, 15]
ORDER = KEPT + [6, 7, 8, 9]


def tables():
    unit = 1.0 / math.sqrt(N)
    wave = np.arange(N)
    wave = np.where(wave < N // 2, wave, wave - N) / (N // 2)
    eye = np.eye(8)
    c_natural = np.arange(64)
    c_zw = np.array([4 * w + z for z in range(4) for w in range(16)])
    c_kept = np.array([4 * w + z for z in range(4) for w in ORDER])
    rows = np.arange(64)

    def angle(left, right, length):
        return 2 * np.pi * ((left[:, None] * right[None, :]) % length) / length

    eighth = np.arange(8)
    turn = np.exp(1j * angle(eighth, eighth, 8)) * unit

    first = []
    for e in range(2):
        part = np.zeros((2, 4, 8, 2, 2, 8, 8))
        for m in range(4):
            for l in range(8):
                v = turn[2 * m + e, l]
                for j in range(8):
                    part[0, m, j, 0, 0, l, j] = v.real
                    part[1, m, j, 0, 0, l, j] = -v.imag
                    part[0, m, j, 0, 1, l, j] = v.imag
                    part[1, m, j, 0, 1, l, j] = v.real
        part[:, :, :, 1, 0] = -part[:, :, :, 0, 1]
        part[:, :, :, 1, 1] = part[:, :, :, 0, 0]
        first.append(part.reshape(64, 256))

    lane = np.arange(128)
    twist_y = angle(rows, (lane // 8) % 8, N)
    twist_x = angle(rows, lane % 8, N)

    mixed = np.zeros((2, 2, 8, 8, 2, 8, 8))
    forward = np.zeros((2, 8, 8, 2, 2, 8, 8))
    last = [np.zeros((2, 2, 8, 8, 2, 4, 8)) for _ in range(2)]
    for l in range(8):
        for j in range(8):
            for p in range(8):
                v = turn[j, p]
                for half in range(2):
                    mixed[0, 0, l, j, half, p, l] = v.real
                    mixed[0, 1, l, j, half, p, l] = -v.imag
                    mixed[1, 0, l, j, half, p, l] = -v.imag
                    mixed[1, 1, l, j, half, p, l] = -v.real
                forward[0, p, l, 0, 0, l, j] = v.real
                forward[0, p, l, 0, 1, l, j] = -v.imag
                forward[0, p, l, 1, 0, l, j] = v.imag
                forward[0, p, l, 1, 1, l, j] = v.real
            for m in range(4):
                for e in range(2):
                    v = turn[2 * m + e, l]
                    t = last[e]
                    t[0, 0, l, j, 0, m, j] = v.real
                    t[1, 1, l, j, 0, m, j] = v.real
                    t[0, 1, l, j, 0, m, j] = v.imag
                    t[1, 0, l, j, 0, m, j] = -v.imag
                    t[0, 1, l, j, 1, m, j] = v.real
                    t[1, 0, l, j, 1, m, j] = -v.real
                    t[0, 0, l, j, 1, m, j] = -v.imag
                    t[1, 1, l, j, 1, m, j] = -v.imag
    forward_y = np.zeros_like(forward)
    forward_y[1] = forward[0]

    def pair(order):
        t = angle(order, rows, 64)
        return np.concatenate([np.cos(t), np.sin(t)], axis=1)

    stacked = angle(rows, c_zw, 64)
    kappa_y = np.zeros((2, 64, 2, 4, 8))
    for e in range(2):
        for m in range(4):
            kappa_y[e, :, :, m, :] = wave[64 * (2 * m + e) + rows][:, None, None]
    kappa_x = wave[8 * c_zw[:, None] + (lane % 8)[None, :]]

    spread = np.zeros((128, 256))
    for f in range(-2, 130):
        k = f // 2 + 1
        if f % 2 == 0:
            spread[k, f % 256] = 1.0
        else:
            spread[k, f % 256] = 0.5
            spread[k + 1, f % 256] = 0.5
    lift = np.zeros((2, 24, 24))
    for v in range(2):
        def slot(row):
            if row < 0:
                return 20 + v
            return 8 * v + row if row < 8 else 16 + 2 * v + row - 8
        for f in range(-2, 18):
            k = f // 2
            if f % 2 == 0:
                lift[v, f + 4, slot(k)] = 1.0
            else:
                lift[v, f + 4, slot(k)] = 0.5
                lift[v, f + 4, slot(k + 1)] = 0.5

    out = dict(
        first0=first[0], first1=first[1],
        tyc=np.cos(twist_y), tys=np.sin(twist_y), txc=np.cos(twist_x), txs=np.sin(twist_x),
        cs1=pair(c_natural), cs3=np.concatenate([np.cos(stacked).T, np.sin(stacked).T]).reshape(2, 64, 64).transpose(0, 1, 2).reshape(128, 64),
        mixed=mixed.reshape(256, 128), fx=forward.reshape(128, 256), fy=forward_y.reshape(128, 256),
        cs4=pair(c_kept), last0=last[0].reshape(256, 64), last1=last[1].reshape(256, 64),
        ky=kappa_y.reshape(128, 64), kx=kappa_x, spread=spread, lift=lift.reshape(48, 24),
    )
    flat = angle(rows, c_zw, 64)
    out["cs3"] = np.concatenate([np.cos(flat), np.sin(flat)], axis=0)
    return {k: np.asarray(v, np.float32) for k, v in out.items()}


NAMES = ["first0", "first1", "tyc", "tys", "txc", "txs", "cs1", "cs3", "mixed", "fx", "fy", "cs4",
         "last0", "last1", "ky", "kx", "spread", "lift"]


def dot(a, b):
    return jnp.dot(a, b, precision=lax.Precision.HIGHEST, preferred_element_type=jnp.float32)


def inverse_y(t, spectra, kappa_x):
    turned = []
    for comp in range(3):
        stacked = jnp.concatenate(
            [spectra(comp, ri)[:, 128 * m : 128 * m + 128] for ri in range(2) for m in range(4)], axis=0
        )
        turned.append(stacked.T)
    spin_x = turned[2] * t["ky"]
    spin_z = turned[1] * kappa_x - turned[0] * t["ky"]
    fields = turned + [spin_x, spin_z]
    even = jnp.concatenate([f[:64] for f in fields], axis=0)
    odd = jnp.concatenate([f[64:] for f in fields], axis=0)
    mixed = dot(even, t["first0"]) + dot(odd, t["first1"])
    upper, lower = [], []
    for n in range(5):
        plain = mixed[64 * n : 64 * n + 64, :128]
        times_i = mixed[64 * n : 64 * n + 64, 128:]
        if n >= 3:
            plain, times_i = times_i, -plain
        upper.append(plain * t["tyc"] + times_i * t["tys"])
        lower.append(times_i * t["tyc"] - plain * t["tys"])
    both = jnp.concatenate([jnp.concatenate(upper, axis=1), jnp.concatenate(lower, axis=1)], axis=0)
    blocks = dot(t["cs1"], both)
    return [blocks[:, 128 * n : 128 * n + 128] for n in range(5)]


def inverse_x(t, blocks):
    u, v, w, spin_x, spin_z = blocks
    six = [u, v, w, spin_x, w * t["kx"], spin_z]
    summed = dot(t["cs3"], jnp.concatenate(six, axis=1))
    rows = []
    for n in range(6):
        first = summed[:64, 128 * n : 128 * n + 128]
        second = summed[64:, 128 * n : 128 * n + 128]
        a = first * t["txc"] - second * t["txs"]
        b = first * t["txs"] + second * t["txc"]
        if n == 4:
            a, b = b, -a
        rows.append(jnp.concatenate([a, b], axis=1))
    fields = dot(jnp.concatenate(rows, axis=0), t["mixed"])
    return [fields[64 * n : 64 * n + 64] for n in range(6)]


def forward_x(t, fields):
    u, v, w, ox, oy, oz = fields
    left = lax.broadcasted_iota(jnp.int32, (64, 128), 1) < 64
    product_xy = jnp.where(left, v, w) * jnp.where(left, oz, ox) - jnp.where(left, w, u) * jnp.where(left, oy, oz)
    product_z = u * oy - v * ox
    mixed = [dot(product_xy, t["fx"]), dot(product_xy, t["fy"]), dot(product_z, t["fx"])]
    upper, lower = [], []
    for m in mixed:
        plain, times_i = m[:, :128], m[:, 128:]
        upper.append(plain * t["txc"] - times_i * t["txs"])
        lower.append(-(times_i * t["txc"] + plain * t["txs"]))
    both = jnp.concatenate([jnp.concatenate(upper, axis=1), jnp.concatenate(lower, axis=1)], axis=0)
    blocks = dot(t["cs4"], both)
    return [blocks[:, 128 * n : 128 * n + 128] for n in range(3)]


def forward_y(t, blocks):
    summed = dot(t["cs3"], jnp.concatenate(blocks, axis=1))
    rows = []
    for n in range(3):
        first = summed[:64, 128 * n : 128 * n + 128]
        second = summed[64:, 128 * n : 128 * n + 128]
        rows.append(
            jnp.concatenate(
                [first * t["tyc"] - second * t["tys"], first * t["tys"] + second * t["tyc"]], axis=1
            )
        )
    rows = jnp.concatenate(rows, axis=0)
    even, odd = dot(rows, t["last0"]), dot(rows, t["last1"])
    return [
        jnp.concatenate([even[64 * n : 64 * n + 64], odd[64 * n : 64 * n + 64]], axis=0).T for n in range(3)
    ]


def kernel(vh, sc, off, *rest):
    t = {name: rest[i] for i, name in enumerate(NAMES)}
    (vnew, snew, send1, recv1, send2, recv2, relay2, send3, recv3, send4, recv4,
     vsend, vrecv, vlo_s, vhi_s, vlo_r, vhi_r, edge_s, edge_r, rim_s, rim_r, corner_s, corner_r, turned, tile, side, coarse, fine,
     s1, r1, s2, r2, s3, r3, s4, r4, sv, rv, sm, rm) = rest[len(NAMES):]
    t = {name: ref[...] for name, ref in t.items()}

    g = lax.axis_index("group")
    r = lax.axis_index("row")
    c = lax.axis_index("col")
    w, z = c // 4, c % 4
    z_up, z_down, z_far = (z + 1) % 4, (z + 3) % 4, (z + 2) % 4
    up, down, opposite = (g, r, 4 * w + z_up), (g, r, 4 * w + z_down), (g, r, 4 * w + z_far)
    c_next, c_prev = (g, r, (c + 1) % 64), (g, r, (c + 63) % 64)
    r_next, r_prev = (g, (r + 1) % 8, c), (g, (r + 7) % 8, c)
    plane_peers = [(g, r, 4 * ((w + d) % 16) + z) for d in range(1, 16)]
    row_peers = [(g, (r + d) % 8, c) for d in range(1, 8)]
    kept = jnp.logical_or(w < 6, w >= 10)

    barrier = pltpu.get_barrier_semaphore()
    greeted = plane_peers + row_peers + [up, down, c_next, c_prev]
    for peer in greeted:
        pl.semaphore_signal(barrier, inc=1, device_id=peer, device_id_type=MESH)

    def remote(src, dst, ssem, rsem, peer):
        return pltpu.make_async_remote_copy(
            src_ref=src, dst_ref=dst, send_sem=ssem, recv_sem=rsem, device_id=peer, device_id_type=MESH
        )

    def rows(ref, start, size):
        return ref.at[pl.ds(pl.multiple_of(start, 8), size), :]

    lane64 = lax.broadcasted_iota(jnp.int32, (1, 64), 1)
    wave = 8 * c + lane64 % 8
    kappa = jnp.where(wave < 256, wave, wave - 512).astype(jnp.float32) * (1.0 / 256.0)
    blocks = inverse_y(t, lambda comp, ri: vh[2 * comp + ri], kappa)
    zero = jnp.zeros((4, 128), jnp.float32)
    for d in range(16):
        part = [b[4 * d : 4 * d + 4] for b in blocks] + [zero]
        send1[24 * d : 24 * d + 24, :] = jnp.concatenate(part, axis=0)

    side[...] = jnp.zeros_like(side)
    coarse[...] = jnp.zeros_like(coarse)
    for p in range(8):
        turned[16 * p : 16 * p + 16, :] = sc[p]
        tile[24 * p + 4 : 24 * p + 20, :] = sc[p]
    flat = turned[...].T
    edge_s[0] = flat[120:128]
    edge_s[1] = flat[0:8]
    for i in range(4):
        rim_s[0, 8 * i : 8 * i + 8, :] = turned[pl.ds(12 + i, 8, stride=16), :]
        rim_s[1, 8 * i : 8 * i + 8, :] = turned[pl.ds(i, 8, stride=16), :]

    pl.semaphore_wait(barrier, len(greeted))

    edge_right = remote(edge_s.at[0], edge_r.at[0], sm.at[0], rm.at[0], r_next)
    edge_left = remote(edge_s.at[1], edge_r.at[1], sm.at[1], rm.at[1], r_prev)
    rim_next = remote(rim_s.at[0], rim_r.at[0], sm.at[2], rm.at[2], c_next)
    rim_prev = remote(rim_s.at[1], rim_r.at[1], sm.at[3], rm.at[3], c_prev)
    edge_right.start()
    edge_left.start()
    sent1 = []
    for d in range(1, 16):
        to = (w + d) % 16
        copy = remote(rows(send1, 24 * to, 24), rows(recv1, 24 * w, 24), s1.at[d], r1.at[d], plane_peers[d - 1])
        copy.start()
        sent1.append(copy)
    rim_next.start()
    rim_prev.start()
    mine = pl.ds(pl.multiple_of(24 * w, 8), 24)
    recv1[mine, :] = send1[mine, :]
    for copy in sent1:
        copy.wait_recv()
    for k in range(4):
        for f in range(5):
            send2[k, 16 * f : 16 * f + 16, :] = recv1[pl.ds(4 * f + k, 16, stride=24), :]

    half = 40
    far_up = remote(send2.at[z_far, pl.ds(0, half)], relay2.at[0], s2.at[0], r2.at[0], up)
    far_down = remote(send2.at[z_far, pl.ds(half, half)], relay2.at[1], s2.at[1], r2.at[1], down)
    near_up = remote(send2.at[z_up], recv2.at[z], s2.at[2], r2.at[2], up)
    near_down = remote(send2.at[z_down], recv2.at[z], s2.at[3], r2.at[3], down)
    far_up.start()
    far_down.start()
    near_up.start()
    near_down.start()
    recv2[z] = send2[z]
    far_up.wait_recv()
    pass_up = remote(relay2.at[0], recv2.at[z_down, pl.ds(0, half)], s2.at[4], r2.at[4], up)
    pass_up.start()
    far_down.wait_recv()
    pass_down = remote(relay2.at[1], recv2.at[z_up, pl.ds(half, half)], s2.at[5], r2.at[5], down)
    pass_down.start()

    edge_right.wait_recv()
    edge_left.wait_recv()
    corner_s[...] = jnp.concatenate(
        [edge_r[1, 0:2, :], edge_r[0, 6:8, :], jnp.zeros((4, 128), jnp.float32)], axis=0
    )
    corner_next = remote(corner_s, corner_r.at[0], sm.at[6], rm.at[6], c_next)
    corner_prev = remote(corner_s, corner_r.at[1], sm.at[7], rm.at[7], c_prev)
    corner_next.start()
    corner_prev.start()
    beside = jnp.concatenate([edge_r[1], jnp.zeros((112, 128), jnp.float32), edge_r[0]], axis=0).T
    for p in range(8):
        side[24 * p + 4 : 24 * p + 20, :] = beside[16 * p : 16 * p + 16]

    near_up.wait_recv()
    near_down.wait_recv()
    pass_up.wait_recv()
    pass_down.wait_recv()

    landed = [
        jnp.concatenate([recv2[k, 16 * f : 16 * f + 16, :] for k in range(4)], axis=0) for f in range(5)
    ]
    fields = inverse_x(t, landed)
    leaving = forward_x(t, fields)
    for k in range(4):
        for f in range(3):
            send3[k, 12 * f : 12 * f + 12, :] = leaving[f][16 * k : 16 * k + 12]
        send3[k, 36:40, :] = zero
    far3 = remote(send3.at[z_far], rows(recv3, 40 * z, 40), s3.at[0], r3.at[0], opposite)
    near_up3 = remote(send3.at[z_up], rows(recv3, 40 * z, 40), s3.at[1], r3.at[1], up)
    near_down3 = remote(send3.at[z_down], rows(recv3, 40 * z, 40), s3.at[2], r3.at[2], down)

    @pl.when(z % 2 == 0)
    def _():
        far3.start()

    near_up3.start()
    near_down3.start()

    @pl.when(z % 2 == 1)
    def _():
        far3.start()

    recv3[pl.ds(pl.multiple_of(40 * z, 8), 40), :] = send3[z]

    left = lax.broadcasted_iota(jnp.int32, (64, 128), 1) < 64
    speeds = jnp.where(left, fields[0], fields[1]).T
    lines = []
    for f in range(2):
        lines.append(
            jnp.concatenate([speeds[64 * f + 8 * p : 64 * f + 8 * p + 8, :] for p in range(8)], axis=1)
        )
    lines = jnp.concatenate(lines, axis=0)
    rolled = pltpu.roll(lines, (513 - off[0]) % 512, 1)
    shifted = pltpu.roll(rolled, 448, 1)
    for k in range(4):
        vsend[2 * k] = rolled[:, 128 * k : 128 * k + 128]
        vsend[2 * k + 1] = shifted[:, 128 * k : 128 * k + 128]
    sentv = []
    for d in range(1, 8):
        copy = remote(vsend.at[(r + d) % 8], rows(vrecv, 16 * r, 16), sv.at[d], rv.at[d], row_peers[d - 1])
        copy.start()
        sentv.append(copy)
    vrecv[pl.ds(pl.multiple_of(16 * r, 8), 16), :] = vsend[r]

    for copy in sentv:
        copy.wait_recv()
    for i, k in enumerate((0, 1, 8, 9)):
        vlo_s[8 * i : 8 * i + 8, :] = vrecv[pl.ds(k, 8, stride=16), :]
    for i, k in enumerate((7, 15)):
        vhi_s[8 * i : 8 * i + 8, :] = vrecv[pl.ds(k, 8, stride=16), :]
    low = remote(vlo_s, vlo_r, sm.at[4], rm.at[4], c_prev)
    high = remote(vhi_s, vhi_r, sm.at[5], rm.at[5], c_next)
    low.start()
    high.start()

    near_up3.wait_recv()
    near_down3.wait_recv()
    far3.wait_recv()

    for k in range(12):
        part = [recv3[pl.ds(12 * f + k, 4, stride=40), :] for f in range(3)] + [zero]
        send4[k] = jnp.concatenate(part, axis=0)
    for d in range(1, 16):
        to = (w + d) % 16
        slot = jnp.where(to < 6, to, to - 4)

        @pl.when(jnp.logical_or(to < 6, to >= 10))
        def _():
            remote(send4.at[slot], rows(recv4, 16 * w, 16), s4.at[d], r4.at[d], plane_peers[d - 1]).start()

    @pl.when(kept)
    def _():
        recv4[pl.ds(pl.multiple_of(16 * w, 8), 16), :] = send4[jnp.where(w < 6, w, w - 4)]

    rim_next.wait_recv()
    rim_prev.wait_recv()
    for i in range(4):
        tile[pl.ds(i, 8, stride=24), :] = rim_r[0, 8 * i : 8 * i + 8, :]
        tile[pl.ds(20 + i, 8, stride=24), :] = rim_r[1, 8 * i : 8 * i + 8, :]
    corner_next.wait_recv()
    corner_prev.wait_recv()
    for n in range(2):
        turned[...] = jnp.concatenate(
            [corner_r[n, 0:2, :], jnp.zeros((124, 128), jnp.float32), corner_r[n, 2:4, :]], axis=0
        ).T
        for i in range(2):
            side[pl.ds(2 + 18 * n + i, 8, stride=24), :] = turned[pl.ds(14 * (1 - n) + i, 8, stride=16), :]
    for p in range(8):
        coarse[24 * p : 24 * p + 16, :] = vrecv[16 * p : 16 * p + 16, :]
    low.wait_recv()
    high.wait_recv()
    for i in range(4):
        coarse[pl.ds(16 + i, 8, stride=24), :] = vlo_r[8 * i : 8 * i + 8, :]
    for i in range(2):
        coarse[pl.ds(20 + i, 8, stride=24), :] = vhi_r[8 * i : 8 * i + 8, :]
    fine[...] = dot(coarse[...], t["spread"])

    def one_plane(p, carry):
        block = pl.ds(pl.multiple_of(24 * p, 8), 24)
        speed = dot(t["lift"], fine[block, :])
        x_speed, y_speed = speed[:24], speed[24:]
        values = jnp.concatenate([tile[block, :], side[block, :]], axis=1)
        for _ in range(2):
            values = advance(values, x_speed, y_speed)
        snew[p] = values[4:20, :128]
        return carry

    lax.fori_loop(0, 8, one_plane, 0)

    row8 = 8 * c + lax.broadcasted_iota(jnp.int32, (8, 128), 0)
    wave_x = jnp.where(row8 < 256, row8, row8 - 512)
    squared_x = jnp.square(wave_x.astype(jnp.float32) * (1.0 / 256.0))
    damping, keep = [], []
    for m in range(4):
        column = 128 * m + lax.broadcasted_iota(jnp.int32, (8, 128), 1)
        wave_y = jnp.where(column < 256, column, column - 512)
        squared_y = jnp.square(wave_y.astype(jnp.float32) * (1.0 / 256.0))
        damping.append(jnp.exp(-viscosity * time_step * (squared_x + squared_y)))
        keep.append(jnp.logical_and(3 * jnp.abs(wave_x) < 512, 3 * jnp.abs(wave_y) < 512))

    @pl.when(jnp.logical_not(kept))
    def _():
        for n in range(6):
            for m in range(4):
                lanes = slice(128 * m, 128 * m + 128)
                vnew[n, :, lanes] = damping[m] * vh[n, :, lanes]

    @pl.when(kept)
    def _():
        for d in range(1, 16):
            remote(send4.at[0], rows(recv4, 0, 16), s4.at[d], r4.at[d], plane_peers[d - 1]).wait_recv()
        gathered = [
            jnp.concatenate([recv4[pl.ds(4 * f + k, 16, stride=16), :] for k in range(4)], axis=0)
            for f in range(3)
        ]
        forcing = forward_y(t, gathered)
        for f in range(3):
            for ri in range(2):
                for m in range(4):
                    lanes = slice(128 * m, 128 * m + 128)
                    push = forcing[f][32 * ri + 8 * m : 32 * ri + 8 * m + 8]
                    n = 2 * f + ri
                    vnew[n, :, lanes] = damping[m] * (
                        vh[n, :, lanes] + time_step * jnp.where(keep[m], push, 0.0)
                    )

    for copy in sent1 + sentv + [
        edge_right, edge_left, rim_next, rim_prev, corner_next, corner_prev, far_up, far_down, near_up, near_down,
        pass_up, pass_down, far3, near_up3, near_down3, low, high,
    ]:
        copy.wait_send()
    for d in range(1, 16):
        to = (w + d) % 16

        @pl.when(jnp.logical_or(to < 6, to >= 10))
        def _():
            remote(send4.at[0], rows(recv4, 0, 16), s4.at[d], r4.at[d], plane_peers[d - 1]).wait_send()


def advance(values, x_speed, y_speed):
    height, breadth = values.shape

    def along(axis, step):
        return pltpu.roll(values, (-step) % values.shape[axis], axis)

    def parts(axis):
        two_back, back, ahead, two_ahead = (along(axis, s) for s in (-2, -1, 1, 2))
        grad = (two_back - two_ahead + 8.0 * (ahead - back)) * (1.0 / 12.0)
        lap = (16.0 * (ahead + back) - two_ahead - two_back - 30.0 * values) * (1.0 / 12.0)
        return grad, lap

    grad_x, lap_x = parts(1)
    grad_y, lap_y = parts(0)
    return values + substep * (diffusivity * (lap_x + lap_y) - (x_speed * grad_x + y_speed * grad_y))


def per_device(velocity_hat, scalar, tile_offset):
    consts = tables()
    f32 = jnp.float32
    vmem = pl.BlockSpec(memory_space=pltpu.VMEM)
    dma = pltpu.SemaphoreType.DMA

    def buf(*shape):
        return pltpu.VMEM(shape, f32)

    vnew, snew = pl.pallas_call(
        kernel,
        name="coupled_step",
        out_shape=(jax.ShapeDtypeStruct((6, 8, 512), f32), jax.ShapeDtypeStruct((8, 16, 128), f32)),
        in_specs=[vmem, vmem, pl.BlockSpec(memory_space=pltpu.SMEM)] + [vmem] * len(NAMES),
        out_specs=(vmem, vmem),
        scratch_shapes=[
            buf(384, 128), buf(384, 128), buf(4, 80, 128), buf(4, 80, 128), buf(2, 40, 128),
            buf(4, 40, 128), buf(160, 128), buf(12, 16, 128), buf(256, 128),
            buf(8, 16, 128), buf(128, 128), buf(32, 128), buf(16, 128), buf(32, 128), buf(16, 128),
            buf(2, 8, 128), buf(2, 8, 128), buf(2, 32, 128), buf(2, 32, 128), buf(8, 128), buf(2, 8, 128), buf(128, 128),
            buf(192, 128), buf(192, 128),
            buf(192, 128), buf(192, 256),
            dma((16,)), dma((16,)), dma((6,)), dma((6,)), dma((3,)), dma((3,)), dma((16,)), dma((16,)),
            dma((8,)), dma((8,)), dma((8,)), dma((8,)),
        ],
        compiler_params=pltpu.CompilerParams(collective_id=0, has_side_effects=True),
    )(velocity_hat.reshape(6, 8, 512), scalar, tile_offset, *[jnp.asarray(consts[k]) for k in NAMES])
    return vnew.reshape(3, 2, 1, 8, 512), snew


def solution(mesh):
    return jax.shard_map(
        per_device,
        mesh=mesh,
        in_specs=(P(None, None, ("group", "row"), "col", None), P("group", "col", "row"), P()),
        out_specs=(P(None, None, ("group", "row"), "col", None), P("group", "col", "row")),
        check_vma=False,
    )
```

```python
import math

import jax
import jax.numpy as jnp
import numpy as np
from jax import lax
from jax.experimental import pallas as pl
from jax.experimental.pallas import tpu as pltpu
from jax.sharding import PartitionSpec as P

time_step = 0.25
viscosity = 2.0
diffusivity = 0.15
substep = 0.2
MESH = pl.DeviceIdType.MESH

N, NC, NL = 512, 64, 8
KEPT = [0, 1, 2, 3, 4, 5, 10, 11, 12, 13, 14, 15]
ORDER = KEPT + [6, 7, 8, 9]


def tables():
    unit = 1.0 / math.sqrt(N)
    wave = np.arange(N)
    wave = np.where(wave < N // 2, wave, wave - N) / (N // 2)
    eye = np.eye(8)
    c_natural = np.arange(64)
    c_zw = np.array([4 * w + z for z in range(4) for w in range(16)])
    c_kept = np.array([4 * w + z for z in range(4) for w in ORDER])
    rows = np.arange(64)

    def angle(left, right, length):
        return 2 * np.pi * ((left[:, None] * right[None, :]) % length) / length

    eighth = np.arange(8)
    turn = np.exp(1j * angle(eighth, eighth, 8)) * unit

    first = []
    for e in range(2):
        part = np.zeros((2, 4, 8, 2, 2, 8, 8))
        for m in range(4):
            for l in range(8):
                v = turn[2 * m + e, l]
                for j in range(8):
                    part[0, m, j, 0, 0, l, j] = v.real
                    part[1, m, j, 0, 0, l, j] = -v.imag
                    part[0, m, j, 0, 1, l, j] = v.imag
                    part[1, m, j, 0, 1, l, j] = v.real
        part[:, :, :, 1, 0] = -part[:, :, :, 0, 1]
        part[:, :, :, 1, 1] = part[:, :, :, 0, 0]
        first.append(part.reshape(64, 256))

    lane = np.arange(128)
    twist_y = angle(rows, (lane // 8) % 8, N)
    twist_x = angle(rows, lane % 8, N)

    mixed = np.zeros((2, 2, 8, 8, 2, 8, 8))
    forward = np.zeros((2, 8, 8, 2, 2, 8, 8))
    last = [np.zeros((2, 2, 8, 8, 2, 4, 8)) for _ in range(2)]
    for l in range(8):
        for j in range(8):
            for p in range(8):
                v = turn[j, p]
                for half in range(2):
                    mixed[0, 0, l, j, half, p, l] = v.real
                    mixed[0, 1, l, j, half, p, l] = -v.imag
                    mixed[1, 0, l, j, half, p, l] = -v.imag
                    mixed[1, 1, l, j, half, p, l] = -v.real
                forward[0, p, l, 0, 0, l, j] = v.real
                forward[0, p, l, 0, 1, l, j] = -v.imag
                forward[0, p, l, 1, 0, l, j] = v.imag
                forward[0, p, l, 1, 1, l, j] = v.real
            for m in range(4):
                for e in range(2):
                    v = turn[2 * m + e, l]
                    t = last[e]
                    t[0, 0, l, j, 0, m, j] = v.real
                    t[1, 1, l, j, 0, m, j] = v.real
                    t[0, 1, l, j, 0, m, j] = v.imag
                    t[1, 0, l, j, 0, m, j] = -v.imag
                    t[0, 1, l, j, 1, m, j] = v.real
                    t[1, 0, l, j, 1, m, j] = -v.real
                    t[0, 0, l, j, 1, m, j] = -v.imag
                    t[1, 1, l, j, 1, m, j] = -v.imag
    forward_y = np.zeros_like(forward)
    forward_y[1] = forward[0]

    def pair(order):
        t = angle(order, rows, 64)
        return np.concatenate([np.cos(t), np.sin(t)], axis=1)

    stacked = angle(rows, c_zw, 64)
    kappa_y = np.zeros((2, 64, 2, 4, 8))
    for e in range(2):
        for m in range(4):
            kappa_y[e, :, :, m, :] = wave[64 * (2 * m + e) + rows][:, None, None]
    kappa_x = wave[8 * c_zw[:, None] + (lane % 8)[None, :]]

    spread = np.zeros((128, 256))
    for f in range(-2, 130):
        k = f // 2 + 1
        if f % 2 == 0:
            spread[k, f % 256] = 1.0
        else:
            spread[k, f % 256] = 0.5
            spread[k + 1, f % 256] = 0.5
    lift = np.zeros((2, 24, 24))
    for v in range(2):
        def slot(row):
            if row < 0:
                return 20 + v
            return 8 * v + row if row < 8 else 16 + 2 * v + row - 8
        for f in range(-2, 18):
            k = f // 2
            if f % 2 == 0:
                lift[v, f + 4, slot(k)] = 1.0
            else:
                lift[v, f + 4, slot(k)] = 0.5
                lift[v, f + 4, slot(k + 1)] = 0.5

    out = dict(
        first0=first[0], first1=first[1],
        tyc=np.cos(twist_y), tys=np.sin(twist_y), txc=np.cos(twist_x), txs=np.sin(twist_x),
        cs1=pair(c_natural), cs3=np.concatenate([np.cos(stacked).T, np.sin(stacked).T]).reshape(2, 64, 64).transpose(0, 1, 2).reshape(128, 64),
        mixed=mixed.reshape(256, 128), fx=forward.reshape(128, 256), fy=forward_y.reshape(128, 256),
        cs4=pair(c_kept), last0=last[0].reshape(256, 64), last1=last[1].reshape(256, 64),
        ky=kappa_y.reshape(128, 64), kx=kappa_x, spread=spread, lift=lift.reshape(48, 24),
    )
    flat = angle(rows, c_zw, 64)
    out["cs3"] = np.concatenate([np.cos(flat), np.sin(flat)], axis=0)
    return {k: np.asarray(v, np.float32) for k, v in out.items()}


NAMES = ["first0", "first1", "tyc", "tys", "txc", "txs", "cs1", "cs3", "mixed", "fx", "fy", "cs4",
         "last0", "last1", "ky", "kx", "spread", "lift"]


def dot(a, b):
    return jnp.dot(a, b, precision=lax.Precision.HIGHEST, preferred_element_type=jnp.float32)


def inverse_y(t, spectra, kappa_x):
    turned = []
    for comp in range(3):
        stacked = jnp.concatenate(
            [spectra(comp, ri)[:, 128 * m : 128 * m + 128] for ri in range(2) for m in range(4)], axis=0
        )
        turned.append(stacked.T)
    spin_x = turned[2] * t["ky"]
    spin_z = turned[1] * kappa_x - turned[0] * t["ky"]
    fields = turned + [spin_x, spin_z]
    even = jnp.concatenate([f[:64] for f in fields], axis=0)
    odd = jnp.concatenate([f[64:] for f in fields], axis=0)
    mixed = dot(even, t["first0"]) + dot(odd, t["first1"])
    upper, lower = [], []
    for n in range(5):
        plain = mixed[64 * n : 64 * n + 64, :128]
        times_i = mixed[64 * n : 64 * n + 64, 128:]
        if n >= 3:
            plain, times_i = times_i, -plain
        upper.append(plain * t["tyc"] + times_i * t["tys"])
        lower.append(times_i * t["tyc"] - plain * t["tys"])
    both = jnp.concatenate([jnp.concatenate(upper, axis=1), jnp.concatenate(lower, axis=1)], axis=0)
    blocks = dot(t["cs1"], both)
    return [blocks[:, 128 * n : 128 * n + 128] for n in range(5)]


def inverse_x(t, blocks):
    u, v, w, spin_x, spin_z = blocks
    six = [u, v, w, spin_x, w * t["kx"], spin_z]
    summed = dot(t["cs3"], jnp.concatenate(six, axis=1))
    rows = []
    for n in range(6):
        first = summed[:64, 128 * n : 128 * n + 128]
        second = summed[64:, 128 * n : 128 * n + 128]
        a = first * t["txc"] - second * t["txs"]
        b = first * t["txs"] + second * t["txc"]
        if n == 4:
            a, b = b, -a
        rows.append(jnp.concatenate([a, b], axis=1))
    fields = dot(jnp.concatenate(rows, axis=0), t["mixed"])
    return [fields[64 * n : 64 * n + 64] for n in range(6)]


def forward_x(t, fields):
    u, v, w, ox, oy, oz = fields
    left = lax.broadcasted_iota(jnp.int32, (64, 128), 1) < 64
    product_xy = jnp.where(left, v, w) * jnp.where(left, oz, ox) - jnp.where(left, w, u) * jnp.where(left, oy, oz)
    product_z = u * oy - v * ox
    mixed = [dot(product_xy, t["fx"]), dot(product_xy, t["fy"]), dot(product_z, t["fx"])]
    upper, lower = [], []
    for m in mixed:
        plain, times_i = m[:, :128], m[:, 128:]
        upper.append(plain * t["txc"] - times_i * t["txs"])
        lower.append(-(times_i * t["txc"] + plain * t["txs"]))
    both = jnp.concatenate([jnp.concatenate(upper, axis=1), jnp.concatenate(lower, axis=1)], axis=0)
    blocks = dot(t["cs4"], both)
    return [blocks[:, 128 * n : 128 * n + 128] for n in range(3)]


def forward_y(t, blocks):
    summed = dot(t["cs3"], jnp.concatenate(blocks, axis=1))
    rows = []
    for n in range(3):
        first = summed[:64, 128 * n : 128 * n + 128]
        second = summed[64:, 128 * n : 128 * n + 128]
        rows.append(
            jnp.concatenate(
                [first * t["tyc"] - second * t["tys"], first * t["tys"] + second * t["tyc"]], axis=1
            )
        )
    rows = jnp.concatenate(rows, axis=0)
    even, odd = dot(rows, t["last0"]), dot(rows, t["last1"])
    return [
        jnp.concatenate([even[64 * n : 64 * n + 64], odd[64 * n : 64 * n + 64]], axis=0).T for n in range(3)
    ]


def kernel(vh, sc, off, *rest):
    t = {name: rest[i] for i, name in enumerate(NAMES)}
    (vnew, snew, send1, recv1, send2, recv2, relay2, send3, recv3, send4, recv4,
     vsend, vrecv, vlo_s, vhi_s, vlo_r, vhi_r, edge_s, edge_r, rim_s, rim_r, corner_s, corner_r, turned, tile, side, coarse, fine,
     s1, r1, s2, r2, s3, r3, s4, r4, sv, rv, sl, rl, sh, rh, sm, rm, row_sem) = rest[len(NAMES):]
    t = {name: ref[...] for name, ref in t.items()}

    g = lax.axis_index("group")
    r = lax.axis_index("row")
    c = lax.axis_index("col")
    w, z = c // 4, c % 4
    z_up, z_down, z_far = (z + 1) % 4, (z + 3) % 4, (z + 2) % 4
    up, down, opposite = (g, r, 4 * w + z_up), (g, r, 4 * w + z_down), (g, r, 4 * w + z_far)
    c_next, c_prev = (g, r, (c + 1) % 64), (g, r, (c + 63) % 64)
    r_next, r_prev = (g, (r + 1) % 8, c), (g, (r + 7) % 8, c)
    plane_peers = [(g, r, 4 * ((w + d) % 16) + z) for d in range(1, 16)]
    row_peers = [(g, (r + d) % 8, c) for d in range(1, 8)]
    kept = jnp.logical_or(w < 6, w >= 10)

    barrier = pltpu.get_barrier_semaphore()
    greeted = plane_peers + row_peers + [up, down, c_next, c_prev]
    for peer in greeted:
        pl.semaphore_signal(barrier, inc=1, device_id=peer, device_id_type=MESH)

    def remote(src, dst, ssem, rsem, peer):
        return pltpu.make_async_remote_copy(
            src_ref=src, dst_ref=dst, send_sem=ssem, recv_sem=rsem, device_id=peer, device_id_type=MESH
        )

    def rows(ref, start, size):
        return ref.at[pl.ds(pl.multiple_of(start, 8), size), :]

    lane64 = lax.broadcasted_iota(jnp.int32, (1, 64), 1)
    wave = 8 * c + lane64 % 8
    kappa = jnp.where(wave < 256, wave, wave - 512).astype(jnp.float32) * (1.0 / 256.0)
    blocks = inverse_y(t, lambda comp, ri: vh[2 * comp + ri], kappa)
    zero = jnp.zeros((4, 128), jnp.float32)
    for d in range(16):
        part = [b[4 * d : 4 * d + 4] for b in blocks] + [zero]
        send1[24 * d : 24 * d + 24, :] = jnp.concatenate(part, axis=0)

    side[...] = jnp.zeros_like(side)
    coarse[...] = jnp.zeros_like(coarse)
    for p in range(8):
        turned[16 * p : 16 * p + 16, :] = sc[p]
        tile[24 * p + 4 : 24 * p + 20, :] = sc[p]
    flat = turned[...].T
    edge_s[0] = flat[120:128]
    edge_s[1] = flat[0:8]
    for i in range(4):
        rim_s[0, 8 * i : 8 * i + 8, :] = turned[pl.ds(12 + i, 8, stride=16), :]
        rim_s[1, 8 * i : 8 * i + 8, :] = turned[pl.ds(i, 8, stride=16), :]

    pl.semaphore_wait(barrier, len(greeted))
    for peer in row_peers:
        pl.semaphore_signal(row_sem, inc=1, device_id=peer, device_id_type=MESH)

    edge_right = remote(edge_s.at[0], edge_r.at[0], sm.at[0], rm.at[0], r_next)
    edge_left = remote(edge_s.at[1], edge_r.at[1], sm.at[1], rm.at[1], r_prev)
    rim_next = remote(rim_s.at[0], rim_r.at[0], sm.at[2], rm.at[2], c_next)
    rim_prev = remote(rim_s.at[1], rim_r.at[1], sm.at[3], rm.at[3], c_prev)
    edge_right.start()
    edge_left.start()
    sent1 = []
    for d in range(1, 16):
        to = (w + d) % 16
        copy = remote(rows(send1, 24 * to, 20), rows(recv1, 24 * w, 20), s1.at[d], r1.at[d], plane_peers[d - 1])
        copy.start()
        sent1.append(copy)
    rim_next.start()
    rim_prev.start()
    mine = pl.ds(pl.multiple_of(24 * w, 8), 24)
    recv1[mine, :] = send1[mine, :]
    for copy in sent1:
        copy.wait_recv()
    for k in range(4):
        for f in range(5):
            send2[k, 16 * f : 16 * f + 16, :] = recv1[pl.ds(4 * f + k, 16, stride=24), :]

    half = 40
    far_up = remote(send2.at[z_far, pl.ds(0, half)], relay2.at[0], s2.at[0], r2.at[0], up)
    far_down = remote(send2.at[z_far, pl.ds(half, half)], relay2.at[1], s2.at[1], r2.at[1], down)
    near_up = remote(send2.at[z_up], recv2.at[z], s2.at[2], r2.at[2], up)
    near_down = remote(send2.at[z_down], recv2.at[z], s2.at[3], r2.at[3], down)
    far_up.start()
    far_down.start()
    near_up.start()
    near_down.start()
    recv2[z] = send2[z]
    far_up.wait_recv()
    pass_up = remote(relay2.at[0], recv2.at[z_down, pl.ds(0, half)], s2.at[4], r2.at[4], up)
    pass_up.start()
    far_down.wait_recv()
    pass_down = remote(relay2.at[1], recv2.at[z_up, pl.ds(half, half)], s2.at[5], r2.at[5], down)
    pass_down.start()

    edge_right.wait_recv()
    edge_left.wait_recv()
    corner_s[...] = jnp.concatenate(
        [edge_r[1, 0:2, :], edge_r[0, 6:8, :], jnp.zeros((4, 128), jnp.float32)], axis=0
    )
    corner_next = remote(corner_s, corner_r.at[0], sm.at[6], rm.at[6], c_next)
    corner_prev = remote(corner_s, corner_r.at[1], sm.at[7], rm.at[7], c_prev)
    corner_next.start()
    corner_prev.start()
    beside = jnp.concatenate([edge_r[1], jnp.zeros((112, 128), jnp.float32), edge_r[0]], axis=0).T
    for p in range(8):
        side[24 * p + 4 : 24 * p + 20, :] = beside[16 * p : 16 * p + 16]

    near_up.wait_recv()
    near_down.wait_recv()
    pass_up.wait_recv()
    pass_down.wait_recv()

    landed = [
        jnp.concatenate([recv2[k, 16 * f : 16 * f + 16, :] for k in range(4)], axis=0) for f in range(5)
    ]
    fields = inverse_x(t, landed)
    leaving = forward_x(t, fields)
    for k in range(4):
        for f in range(3):
            send3[k, 12 * f : 12 * f + 12, :] = leaving[f][16 * k : 16 * k + 12]
        send3[k, 36:40, :] = zero
    kept_rows = pl.ds(0, 36)
    far3 = remote(send3.at[z_far, kept_rows], rows(recv3, 40 * z, 36), s3.at[0], r3.at[0], opposite)
    near_up3 = remote(send3.at[z_up, kept_rows], rows(recv3, 40 * z, 36), s3.at[1], r3.at[1], up)
    near_down3 = remote(send3.at[z_down, kept_rows], rows(recv3, 40 * z, 36), s3.at[2], r3.at[2], down)

    @pl.when(z % 2 == 0)
    def _():
        far3.start()

    near_up3.start()
    near_down3.start()

    @pl.when(z % 2 == 1)
    def _():
        far3.start()

    recv3[pl.ds(pl.multiple_of(40 * z, 8), 40), :] = send3[z]

    left = lax.broadcasted_iota(jnp.int32, (64, 128), 1) < 64
    speeds = jnp.where(left, fields[0], fields[1]).T
    lines = []
    for f in range(2):
        lines.append(
            jnp.concatenate([speeds[64 * f + 8 * p : 64 * f + 8 * p + 8, :] for p in range(8)], axis=1)
        )
    lines = jnp.concatenate(lines, axis=0)
    rolled = pltpu.roll(lines, (513 - off[0]) % 512, 1)
    shifted = pltpu.roll(rolled, 448, 1)
    for k in range(4):
        vsend[2 * k] = rolled[:, 128 * k : 128 * k + 128]
        vsend[2 * k + 1] = shifted[:, 128 * k : 128 * k + 128]
        for n, source in enumerate((rolled, shifted)):
            part = source[:, 128 * k : 128 * k + 128]
            vlo_s[2 * k + n] = jnp.concatenate([part[0:2], part[8:10], zero], axis=0)
            vhi_s[2 * k + n] = jnp.concatenate([part[7:8], part[15:16], zero, zero[:2]], axis=0)
    pl.semaphore_wait(row_sem, 7)
    sentv = []
    for d in range(1, 8):
        copy = remote(vsend.at[(r + d) % 8], rows(vrecv, 16 * r, 16), sv.at[d], rv.at[d], row_peers[d - 1])
        copy.start()
        sentv.append(copy)
    sentr = []
    for d in range(8):
        to = (r + d) % 8
        low = remote(vlo_s.at[to, pl.ds(0, 4)], vlo_r.at[r, pl.ds(0, 4)], sl.at[d], rl.at[d], (g, to, (c + 63) % 64))
        high = remote(vhi_s.at[to, pl.ds(0, 2)], vhi_r.at[r, pl.ds(0, 2)], sh.at[d], rh.at[d], (g, to, (c + 1) % 64))
        low.start()
        high.start()
        sentr += [low, high]
    vrecv[pl.ds(pl.multiple_of(16 * r, 8), 16), :] = vsend[r]

    near_up3.wait_recv()
    near_down3.wait_recv()
    far3.wait_recv()

    for k in range(12):
        part = [recv3[pl.ds(12 * f + k, 4, stride=40), :] for f in range(3)] + [zero]
        send4[k] = jnp.concatenate(part, axis=0)
    for d in range(1, 16):
        to = (w + d) % 16
        slot = jnp.where(to < 6, to, to - 4)

        @pl.when(jnp.logical_or(to < 6, to >= 10))
        def _():
            remote(send4.at[slot], rows(recv4, 16 * w, 16), s4.at[d], r4.at[d], plane_peers[d - 1]).start()

    @pl.when(kept)
    def _():
        recv4[pl.ds(pl.multiple_of(16 * w, 8), 16), :] = send4[jnp.where(w < 6, w, w - 4)]

    rim_next.wait_recv()
    rim_prev.wait_recv()
    for i in range(4):
        tile[pl.ds(i, 8, stride=24), :] = rim_r[0, 8 * i : 8 * i + 8, :]
        tile[pl.ds(20 + i, 8, stride=24), :] = rim_r[1, 8 * i : 8 * i + 8, :]
    corner_next.wait_recv()
    corner_prev.wait_recv()
    for n in range(2):
        turned[...] = jnp.concatenate(
            [corner_r[n, 0:2, :], jnp.zeros((124, 128), jnp.float32), corner_r[n, 2:4, :]], axis=0
        ).T
        for i in range(2):
            side[pl.ds(2 + 18 * n + i, 8, stride=24), :] = turned[pl.ds(14 * (1 - n) + i, 8, stride=16), :]
    for copy in sentv + sentr:
        copy.wait_recv()
    for p in range(8):
        coarse[24 * p : 24 * p + 16, :] = vrecv[16 * p : 16 * p + 16, :]
        coarse[24 * p + 16 : 24 * p + 20, :] = vlo_r[p, 0:4, :]
        coarse[24 * p + 20 : 24 * p + 22, :] = vhi_r[p, 0:2, :]
    fine[...] = dot(coarse[...], t["spread"])

    def one_plane(p, carry):
        block = pl.ds(pl.multiple_of(24 * p, 8), 24)
        speed = dot(t["lift"], fine[block, :])
        x_speed, y_speed = speed[:24], speed[24:]
        values = jnp.concatenate([tile[block, :], side[block, :]], axis=1)
        for _ in range(2):
            values = advance(values, x_speed, y_speed)
        snew[p] = values[4:20, :128]
        return carry

    lax.fori_loop(0, 8, one_plane, 0)

    row8 = 8 * c + lax.broadcasted_iota(jnp.int32, (8, 128), 0)
    wave_x = jnp.where(row8 < 256, row8, row8 - 512)
    squared_x = jnp.square(wave_x.astype(jnp.float32) * (1.0 / 256.0))
    damping, keep = [], []
    for m in range(4):
        column = 128 * m + lax.broadcasted_iota(jnp.int32, (8, 128), 1)
        wave_y = jnp.where(column < 256, column, column - 512)
        squared_y = jnp.square(wave_y.astype(jnp.float32) * (1.0 / 256.0))
        damping.append(jnp.exp(-viscosity * time_step * (squared_x + squared_y)))
        keep.append(jnp.logical_and(3 * jnp.abs(wave_x) < 512, 3 * jnp.abs(wave_y) < 512))

    @pl.when(jnp.logical_not(kept))
    def _():
        for n in range(6):
            for m in range(4):
                lanes = slice(128 * m, 128 * m + 128)
                vnew[n, :, lanes] = damping[m] * vh[n, :, lanes]

    @pl.when(kept)
    def _():
        for d in range(1, 16):
            remote(send4.at[0], rows(recv4, 0, 16), s4.at[d], r4.at[d], plane_peers[d - 1]).wait_recv()
        gathered = [
            jnp.concatenate([recv4[pl.ds(4 * f + k, 16, stride=16), :] for k in range(4)], axis=0)
            for f in range(3)
        ]
        forcing = forward_y(t, gathered)
        for f in range(3):
            for ri in range(2):
                for m in range(4):
                    lanes = slice(128 * m, 128 * m + 128)
                    push = forcing[f][32 * ri + 8 * m : 32 * ri + 8 * m + 8]
                    n = 2 * f + ri
                    vnew[n, :, lanes] = damping[m] * (
                        vh[n, :, lanes] + time_step * jnp.where(keep[m], push, 0.0)
                    )

    for copy in sent1 + sentv + [
        edge_right, edge_left, rim_next, rim_prev, corner_next, corner_prev, far_up, far_down, near_up, near_down,
        pass_up, pass_down, far3, near_up3, near_down3,
    ] + sentr:
        copy.wait_send()
    for d in range(1, 16):
        to = (w + d) % 16

        @pl.when(jnp.logical_or(to < 6, to >= 10))
        def _():
            remote(send4.at[0], rows(recv4, 0, 16), s4.at[d], r4.at[d], plane_peers[d - 1]).wait_send()


def advance(values, x_speed, y_speed):
    height, breadth = values.shape

    def along(axis, step):
        return pltpu.roll(values, (-step) % values.shape[axis], axis)

    def parts(axis):
        two_back, back, ahead, two_ahead = (along(axis, s) for s in (-2, -1, 1, 2))
        grad = (two_back - two_ahead + 8.0 * (ahead - back)) * (1.0 / 12.0)
        lap = (16.0 * (ahead + back) - two_ahead - two_back - 30.0 * values) * (1.0 / 12.0)
        return grad, lap

    grad_x, lap_x = parts(1)
    grad_y, lap_y = parts(0)
    return values + substep * (diffusivity * (lap_x + lap_y) - (x_speed * grad_x + y_speed * grad_y))


def per_device(velocity_hat, scalar, tile_offset):
    consts = tables()
    f32 = jnp.float32
    vmem = pl.BlockSpec(memory_space=pltpu.VMEM)
    dma = pltpu.SemaphoreType.DMA

    def buf(*shape):
        return pltpu.VMEM(shape, f32)

    vnew, snew = pl.pallas_call(
        kernel,
        name="coupled_step",
        out_shape=(jax.ShapeDtypeStruct((6, 8, 512), f32), jax.ShapeDtypeStruct((8, 16, 128), f32)),
        in_specs=[vmem, vmem, pl.BlockSpec(memory_space=pltpu.SMEM)] + [vmem] * len(NAMES),
        out_specs=(vmem, vmem),
        scratch_shapes=[
            buf(384, 128), buf(384, 128), buf(4, 80, 128), buf(4, 80, 128), buf(2, 40, 128),
            buf(4, 40, 128), buf(160, 128), buf(12, 16, 128), buf(256, 128),
            buf(8, 16, 128), buf(128, 128), buf(8, 8, 128), buf(8, 8, 128), buf(8, 8, 128), buf(8, 8, 128),
            buf(2, 8, 128), buf(2, 8, 128), buf(2, 32, 128), buf(2, 32, 128), buf(8, 128), buf(2, 8, 128), buf(128, 128),
            buf(192, 128), buf(192, 128),
            buf(192, 128), buf(192, 256),
            dma((16,)), dma((16,)), dma((6,)), dma((6,)), dma((3,)), dma((3,)), dma((16,)), dma((16,)),
            dma((8,)), dma((8,)), dma((8,)), dma((8,)), dma((8,)), dma((8,)), dma((8,)), dma((8,)),
            pltpu.SemaphoreType.REGULAR,
        ],
        compiler_params=pltpu.CompilerParams(collective_id=0, has_side_effects=True),
    )(velocity_hat.reshape(6, 8, 512), scalar, tile_offset, *[jnp.asarray(consts[k]) for k in NAMES])
    return vnew.reshape(3, 2, 1, 8, 512), snew


def solution(mesh):
    return jax.shard_map(
        per_device,
        mesh=mesh,
        in_specs=(P(None, None, ("group", "row"), "col", None), P("group", "col", "row"), P()),
        out_specs=(P(None, None, ("group", "row"), "col", None), P("group", "col", "row")),
        check_vma=False,
    )
```

```python
import math

import jax
import jax.numpy as jnp
import numpy as np
from jax import lax
from jax.experimental import pallas as pl
from jax.experimental.pallas import tpu as pltpu
from jax.sharding import PartitionSpec as P

time_step = 0.25
viscosity = 2.0
diffusivity = 0.15
substep = 0.2
MESH = pl.DeviceIdType.MESH

N, NC, NL = 512, 64, 8
KEPT = [0, 1, 2, 3, 4, 5, 10, 11, 12, 13, 14, 15]
ORDER = KEPT + [6, 7, 8, 9]


def tables():
    unit = 1.0 / math.sqrt(N)
    wave = np.arange(N)
    wave = np.where(wave < N // 2, wave, wave - N) / (N // 2)
    eye = np.eye(8)
    c_natural = np.arange(64)
    c_zw = np.array([4 * w + z for z in range(4) for w in range(16)])
    c_kept = np.array([4 * w + z for z in range(4) for w in ORDER])
    rows = np.arange(64)

    def angle(left, right, length):
        return 2 * np.pi * ((left[:, None] * right[None, :]) % length) / length

    eighth = np.arange(8)
    turn = np.exp(1j * angle(eighth, eighth, 8)) * unit

    first = []
    for e in range(2):
        part = np.zeros((2, 4, 8, 2, 2, 8, 8))
        for m in range(4):
            for l in range(8):
                v = turn[2 * m + e, l]
                for j in range(8):
                    part[0, m, j, 0, 0, l, j] = v.real
                    part[1, m, j, 0, 0, l, j] = -v.imag
                    part[0, m, j, 0, 1, l, j] = v.imag
                    part[1, m, j, 0, 1, l, j] = v.real
        part[:, :, :, 1, 0] = -part[:, :, :, 0, 1]
        part[:, :, :, 1, 1] = part[:, :, :, 0, 0]
        first.append(part.reshape(64, 256))

    lane = np.arange(128)
    twist_y = angle(rows, (lane // 8) % 8, N)
    twist_x = angle(rows, lane % 8, N)

    mixed = np.zeros((2, 2, 8, 8, 2, 8, 8))
    forward = np.zeros((2, 8, 8, 2, 2, 8, 8))
    last = [np.zeros((2, 2, 8, 8, 2, 4, 8)) for _ in range(2)]
    for l in range(8):
        for j in range(8):
            for p in range(8):
                v = turn[j, p]
                for half in range(2):
                    mixed[0, 0, l, j, half, p, l] = v.real
                    mixed[0, 1, l, j, half, p, l] = -v.imag
                    mixed[1, 0, l, j, half, p, l] = -v.imag
                    mixed[1, 1, l, j, half, p, l] = -v.real
                forward[0, p, l, 0, 0, l, j] = v.real
                forward[0, p, l, 0, 1, l, j] = -v.imag
                forward[0, p, l, 1, 0, l, j] = v.imag
                forward[0, p, l, 1, 1, l, j] = v.real
            for m in range(4):
                for e in range(2):
                    v = turn[2 * m + e, l]
                    t = last[e]
                    t[0, 0, l, j, 0, m, j] = v.real
                    t[1, 1, l, j, 0, m, j] = v.real
                    t[0, 1, l, j, 0, m, j] = v.imag
                    t[1, 0, l, j, 0, m, j] = -v.imag
                    t[0, 1, l, j, 1, m, j] = v.real
                    t[1, 0, l, j, 1, m, j] = -v.real
                    t[0, 0, l, j, 1, m, j] = -v.imag
                    t[1, 1, l, j, 1, m, j] = -v.imag
    forward_y = np.zeros_like(forward)
    forward_y[1] = forward[0]

    def pair(order):
        t = angle(order, rows, 64)
        return np.concatenate([np.cos(t), np.sin(t)], axis=1)

    stacked = angle(rows, c_zw, 64)
    kappa_y = np.zeros((2, 64, 2, 4, 8))
    for e in range(2):
        for m in range(4):
            kappa_y[e, :, :, m, :] = wave[64 * (2 * m + e) + rows][:, None, None]
    kappa_x = wave[8 * c_zw[:, None] + (lane % 8)[None, :]]

    spread = np.zeros((128, 256))
    for f in range(-2, 130):
        k = f // 2 + 1
        if f % 2 == 0:
            spread[k, f % 256] = 1.0
        else:
            spread[k, f % 256] = 0.5
            spread[k + 1, f % 256] = 0.5
    lift = np.zeros((2, 24, 24))
    for v in range(2):
        def slot(row):
            if row < 0:
                return 20 + v
            return 8 * v + row if row < 8 else 16 + 2 * v + row - 8
        for f in range(-2, 18):
            k = f // 2
            if f % 2 == 0:
                lift[v, f + 4, slot(k)] = 1.0
            else:
                lift[v, f + 4, slot(k)] = 0.5
                lift[v, f + 4, slot(k + 1)] = 0.5

    out = dict(
        first0=first[0], first1=first[1],
        tyc=np.cos(twist_y), tys=np.sin(twist_y), txc=np.cos(twist_x), txs=np.sin(twist_x),
        cs1=pair(c_natural), cs3=np.concatenate([np.cos(stacked).T, np.sin(stacked).T]).reshape(2, 64, 64).transpose(0, 1, 2).reshape(128, 64),
        mixed=mixed.reshape(256, 128), fx=forward.reshape(128, 256), fy=forward_y.reshape(128, 256),
        cs4=pair(c_kept), last0=last[0].reshape(256, 64), last1=last[1].reshape(256, 64),
        ky=kappa_y.reshape(128, 64), kx=kappa_x, spread=spread, lift=lift.reshape(48, 24),
    )
    flat = angle(rows, c_zw, 64)
    out["cs3"] = np.concatenate([np.cos(flat), np.sin(flat)], axis=0)
    return {k: np.asarray(v, np.float32) for k, v in out.items()}


NAMES = ["first0", "first1", "tyc", "tys", "txc", "txs", "cs1", "cs3", "mixed", "fx", "fy", "cs4",
         "last0", "last1", "ky", "kx", "spread", "lift"]


def split(a):
    high = a.astype(jnp.bfloat16)
    return high, (a - high.astype(jnp.float32)).astype(jnp.bfloat16)


def dot(a, b):
    (a_high, a_low), (b_high, b_low) = split(a), split(b)

    def product(x, y):
        return jnp.dot(x, y, preferred_element_type=jnp.float32)

    return product(a_high, b_high) + (product(a_high, b_low) + product(a_low, b_high))


def inverse_y(t, spectra, kappa_x):
    turned = []
    for comp in range(3):
        stacked = jnp.concatenate(
            [spectra(comp, ri)[:, 128 * m : 128 * m + 128] for ri in range(2) for m in range(4)], axis=0
        )
        turned.append(stacked.T)
    spin_x = turned[2] * t["ky"]
    spin_z = turned[1] * kappa_x - turned[0] * t["ky"]
    fields = turned + [spin_x, spin_z]
    even = jnp.concatenate([f[:64] for f in fields], axis=0)
    odd = jnp.concatenate([f[64:] for f in fields], axis=0)
    mixed = dot(even, t["first0"]) + dot(odd, t["first1"])
    upper, lower = [], []
    for n in range(5):
        plain = mixed[64 * n : 64 * n + 64, :128]
        times_i = mixed[64 * n : 64 * n + 64, 128:]
        if n >= 3:
            plain, times_i = times_i, -plain
        upper.append(plain * t["tyc"] + times_i * t["tys"])
        lower.append(times_i * t["tyc"] - plain * t["tys"])
    both = jnp.concatenate([jnp.concatenate(upper, axis=1), jnp.concatenate(lower, axis=1)], axis=0)
    blocks = dot(t["cs1"], both)
    return [blocks[:, 128 * n : 128 * n + 128] for n in range(5)]


def inverse_x(t, blocks):
    u, v, w, spin_x, spin_z = blocks
    six = [u, v, w, spin_x, w * t["kx"], spin_z]
    summed = dot(t["cs3"], jnp.concatenate(six, axis=1))
    rows = []
    for n in range(6):
        first = summed[:64, 128 * n : 128 * n + 128]
        second = summed[64:, 128 * n : 128 * n + 128]
        a = first * t["txc"] - second * t["txs"]
        b = first * t["txs"] + second * t["txc"]
        if n == 4:
            a, b = b, -a
        rows.append(jnp.concatenate([a, b], axis=1))
    fields = dot(jnp.concatenate(rows, axis=0), t["mixed"])
    return [fields[64 * n : 64 * n + 64] for n in range(6)]


def forward_x(t, fields):
    u, v, w, ox, oy, oz = fields
    left = lax.broadcasted_iota(jnp.int32, (64, 128), 1) < 64
    product_xy = jnp.where(left, v, w) * jnp.where(left, oz, ox) - jnp.where(left, w, u) * jnp.where(left, oy, oz)
    product_z = u * oy - v * ox
    mixed = [dot(product_xy, t["fx"]), dot(product_xy, t["fy"]), dot(product_z, t["fx"])]
    upper, lower = [], []
    for m in mixed:
        plain, times_i = m[:, :128], m[:, 128:]
        upper.append(plain * t["txc"] - times_i * t["txs"])
        lower.append(-(times_i * t["txc"] + plain * t["txs"]))
    both = jnp.concatenate([jnp.concatenate(upper, axis=1), jnp.concatenate(lower, axis=1)], axis=0)
    blocks = dot(t["cs4"], both)
    return [blocks[:, 128 * n : 128 * n + 128] for n in range(3)]


def forward_y(t, blocks):
    summed = dot(t["cs3"], jnp.concatenate(blocks, axis=1))
    rows = []
    for n in range(3):
        first = summed[:64, 128 * n : 128 * n + 128]
        second = summed[64:, 128 * n : 128 * n + 128]
        rows.append(
            jnp.concatenate(
                [first * t["tyc"] - second * t["tys"], first * t["tys"] + second * t["tyc"]], axis=1
            )
        )
    rows = jnp.concatenate(rows, axis=0)
    even, odd = dot(rows, t["last0"]), dot(rows, t["last1"])
    return [
        jnp.concatenate([even[64 * n : 64 * n + 64], odd[64 * n : 64 * n + 64]], axis=0).T for n in range(3)
    ]


def kernel(vh_far, sc_far, off, *rest):
    n_tables = len(NAMES)
    far_tables, near_tables = rest[:n_tables], rest[-n_tables:]
    rest = rest[:-n_tables]
    (vnew, snew, send1, recv1, send2, recv2, relay2, send3, recv3, send4, recv4,
     vsend, vrecv, vlo_s, vhi_s, vlo_r, vhi_r, edge_s, edge_r, rim_s, rim_r, corner_s, corner_r, turned, tile, side, coarse, fine,
     s1, r1, s2, r2, s3, r3, s4, r4, sv, rv, sl, rl, sh, rh, sm, rm, row_sem, vh, sc, load) = rest[n_tables:]

    g = lax.axis_index("group")
    r = lax.axis_index("row")
    c = lax.axis_index("col")
    w, z = c // 4, c % 4
    z_up, z_down, z_far = (z + 1) % 4, (z + 3) % 4, (z + 2) % 4
    up, down, opposite = (g, r, 4 * w + z_up), (g, r, 4 * w + z_down), (g, r, 4 * w + z_far)
    c_next, c_prev = (g, r, (c + 1) % 64), (g, r, (c + 63) % 64)
    r_next, r_prev = (g, (r + 1) % 8, c), (g, (r + 7) % 8, c)
    plane_peers = [(g, r, 4 * ((w + d) % 16) + z) for d in range(1, 16)]
    row_peers = [(g, (r + d) % 8, c) for d in range(1, 8)]
    kept = jnp.logical_or(w < 6, w >= 10)

    barrier = pltpu.get_barrier_semaphore()
    greeted = plane_peers + row_peers + [up, down, c_next, c_prev]
    for peer in greeted:
        pl.semaphore_signal(barrier, inc=1, device_id=peer, device_id_type=MESH)

    fetched = [pltpu.make_async_copy(vh_far, vh, load.at[0]), pltpu.make_async_copy(sc_far, sc, load.at[1])]
    for n in range(n_tables):
        fetched.append(pltpu.make_async_copy(far_tables[n], near_tables[n], load.at[2 + n]))
    for copy in fetched:
        copy.start()
    for copy in fetched:
        copy.wait()
    t = {name: near_tables[n][...] for n, name in enumerate(NAMES)}

    def remote(src, dst, ssem, rsem, peer):
        return pltpu.make_async_remote_copy(
            src_ref=src, dst_ref=dst, send_sem=ssem, recv_sem=rsem, device_id=peer, device_id_type=MESH
        )

    def rows(ref, start, size):
        return ref.at[pl.ds(pl.multiple_of(start, 8), size), :]

    lane64 = lax.broadcasted_iota(jnp.int32, (1, 64), 1)
    wave = 8 * c + lane64 % 8
    kappa = jnp.where(wave < 256, wave, wave - 512).astype(jnp.float32) * (1.0 / 256.0)
    blocks = inverse_y(t, lambda comp, ri: vh[2 * comp + ri], kappa)
    zero = jnp.zeros((4, 128), jnp.float32)
    for d in range(16):
        part = [b[4 * d : 4 * d + 4] for b in blocks] + [zero]
        send1[24 * d : 24 * d + 24, :] = jnp.concatenate(part, axis=0)

    side[...] = jnp.zeros_like(side)
    coarse[...] = jnp.zeros_like(coarse)
    for p in range(8):
        turned[16 * p : 16 * p + 16, :] = sc[p]
        tile[24 * p + 4 : 24 * p + 20, :] = sc[p]
    flat = turned[...].T
    edge_s[0] = flat[120:128]
    edge_s[1] = flat[0:8]
    for i in range(4):
        rim_s[0, 8 * i : 8 * i + 8, :] = turned[pl.ds(12 + i, 8, stride=16), :]
        rim_s[1, 8 * i : 8 * i + 8, :] = turned[pl.ds(i, 8, stride=16), :]

    pl.semaphore_wait(barrier, len(greeted))
    for peer in row_peers:
        pl.semaphore_signal(row_sem, inc=1, device_id=peer, device_id_type=MESH)

    edge_right = remote(edge_s.at[0], edge_r.at[0], sm.at[0], rm.at[0], r_next)
    edge_left = remote(edge_s.at[1], edge_r.at[1], sm.at[1], rm.at[1], r_prev)
    rim_next = remote(rim_s.at[0], rim_r.at[0], sm.at[2], rm.at[2], c_next)
    rim_prev = remote(rim_s.at[1], rim_r.at[1], sm.at[3], rm.at[3], c_prev)
    edge_right.start()
    edge_left.start()
    sent1 = []
    for d in range(1, 16):
        to = (w + d) % 16
        copy = remote(rows(send1, 24 * to, 20), rows(recv1, 24 * w, 20), s1.at[d], r1.at[d], plane_peers[d - 1])
        copy.start()
        sent1.append(copy)
    rim_next.start()
    rim_prev.start()
    mine = pl.ds(pl.multiple_of(24 * w, 8), 24)
    recv1[mine, :] = send1[mine, :]
    for copy in sent1:
        copy.wait_recv()
    for k in range(4):
        for f in range(5):
            send2[k, 16 * f : 16 * f + 16, :] = recv1[pl.ds(4 * f + k, 16, stride=24), :]

    half = 40
    far_up = remote(send2.at[z_far, pl.ds(0, half)], relay2.at[0], s2.at[0], r2.at[0], up)
    far_down = remote(send2.at[z_far, pl.ds(half, half)], relay2.at[1], s2.at[1], r2.at[1], down)
    near_up = remote(send2.at[z_up], recv2.at[z], s2.at[2], r2.at[2], up)
    near_down = remote(send2.at[z_down], recv2.at[z], s2.at[3], r2.at[3], down)
    far_up.start()
    far_down.start()
    near_up.start()
    near_down.start()
    recv2[z] = send2[z]
    far_up.wait_recv()
    pass_up = remote(relay2.at[0], recv2.at[z_down, pl.ds(0, half)], s2.at[4], r2.at[4], up)
    pass_up.start()
    far_down.wait_recv()
    pass_down = remote(relay2.at[1], recv2.at[z_up, pl.ds(half, half)], s2.at[5], r2.at[5], down)
    pass_down.start()

    edge_right.wait_recv()
    edge_left.wait_recv()
    corner_s[...] = jnp.concatenate(
        [edge_r[1, 0:2, :], edge_r[0, 6:8, :], jnp.zeros((4, 128), jnp.float32)], axis=0
    )
    corner_next = remote(corner_s, corner_r.at[0], sm.at[6], rm.at[6], c_next)
    corner_prev = remote(corner_s, corner_r.at[1], sm.at[7], rm.at[7], c_prev)
    corner_next.start()
    corner_prev.start()
    beside = jnp.concatenate([edge_r[1], jnp.zeros((112, 128), jnp.float32), edge_r[0]], axis=0).T
    for p in range(8):
        side[24 * p + 4 : 24 * p + 20, :] = beside[16 * p : 16 * p + 16]

    near_up.wait_recv()
    near_down.wait_recv()
    pass_up.wait_recv()
    pass_down.wait_recv()

    landed = [
        jnp.concatenate([recv2[k, 16 * f : 16 * f + 16, :] for k in range(4)], axis=0) for f in range(5)
    ]
    fields = inverse_x(t, landed)
    leaving = forward_x(t, fields)
    for k in range(4):
        for f in range(3):
            send3[k, 12 * f : 12 * f + 12, :] = leaving[f][16 * k : 16 * k + 12]
        send3[k, 36:40, :] = zero
    kept_rows = pl.ds(0, 36)
    far3 = remote(send3.at[z_far, kept_rows], rows(recv3, 40 * z, 36), s3.at[0], r3.at[0], opposite)
    near_up3 = remote(send3.at[z_up, kept_rows], rows(recv3, 40 * z, 36), s3.at[1], r3.at[1], up)
    near_down3 = remote(send3.at[z_down, kept_rows], rows(recv3, 40 * z, 36), s3.at[2], r3.at[2], down)

    @pl.when(z % 2 == 0)
    def _():
        far3.start()

    near_up3.start()
    near_down3.start()

    @pl.when(z % 2 == 1)
    def _():
        far3.start()

    recv3[pl.ds(pl.multiple_of(40 * z, 8), 40), :] = send3[z]

    left = lax.broadcasted_iota(jnp.int32, (64, 128), 1) < 64
    speeds = jnp.where(left, fields[0], fields[1]).T
    lines = []
    for f in range(2):
        lines.append(
            jnp.concatenate([speeds[64 * f + 8 * p : 64 * f + 8 * p + 8, :] for p in range(8)], axis=1)
        )
    lines = jnp.concatenate(lines, axis=0)
    rolled = pltpu.roll(lines, (513 - off[0]) % 512, 1)
    shifted = pltpu.roll(rolled, 448, 1)
    for k in range(4):
        vsend[2 * k] = rolled[:, 128 * k : 128 * k + 128]
        vsend[2 * k + 1] = shifted[:, 128 * k : 128 * k + 128]
        for n, source in enumerate((rolled, shifted)):
            part = source[:, 128 * k : 128 * k + 128]
            vlo_s[2 * k + n] = jnp.concatenate([part[0:2], part[8:10], zero], axis=0)
            vhi_s[2 * k + n] = jnp.concatenate([part[7:8], part[15:16], zero, zero[:2]], axis=0)
    pl.semaphore_wait(row_sem, 7)
    sentv = []
    for d in range(1, 8):
        copy = remote(vsend.at[(r + d) % 8], rows(vrecv, 16 * r, 16), sv.at[d], rv.at[d], row_peers[d - 1])
        copy.start()
        sentv.append(copy)
    sentr = []
    for d in range(8):
        to = (r + d) % 8
        low = remote(vlo_s.at[to, pl.ds(0, 4)], vlo_r.at[r, pl.ds(0, 4)], sl.at[d], rl.at[d], (g, to, (c + 63) % 64))
        high = remote(vhi_s.at[to, pl.ds(0, 2)], vhi_r.at[r, pl.ds(0, 2)], sh.at[d], rh.at[d], (g, to, (c + 1) % 64))
        low.start()
        high.start()
        sentr += [low, high]
    vrecv[pl.ds(pl.multiple_of(16 * r, 8), 16), :] = vsend[r]

    near_up3.wait_recv()
    near_down3.wait_recv()
    far3.wait_recv()

    for k in range(12):
        part = [recv3[pl.ds(12 * f + k, 4, stride=40), :] for f in range(3)] + [zero]
        send4[k] = jnp.concatenate(part, axis=0)
    for d in range(1, 16):
        to = (w + d) % 16
        slot = jnp.where(to < 6, to, to - 4)

        @pl.when(jnp.logical_or(to < 6, to >= 10))
        def _():
            remote(send4.at[slot], rows(recv4, 16 * w, 16), s4.at[d], r4.at[d], plane_peers[d - 1]).start()

    @pl.when(kept)
    def _():
        recv4[pl.ds(pl.multiple_of(16 * w, 8), 16), :] = send4[jnp.where(w < 6, w, w - 4)]

    rim_next.wait_recv()
    rim_prev.wait_recv()
    for i in range(4):
        tile[pl.ds(i, 8, stride=24), :] = rim_r[0, 8 * i : 8 * i + 8, :]
        tile[pl.ds(20 + i, 8, stride=24), :] = rim_r[1, 8 * i : 8 * i + 8, :]
    corner_next.wait_recv()
    corner_prev.wait_recv()
    for n in range(2):
        turned[...] = jnp.concatenate(
            [corner_r[n, 0:2, :], jnp.zeros((124, 128), jnp.float32), corner_r[n, 2:4, :]], axis=0
        ).T
        for i in range(2):
            side[pl.ds(2 + 18 * n + i, 8, stride=24), :] = turned[pl.ds(14 * (1 - n) + i, 8, stride=16), :]
    for copy in sentv + sentr:
        copy.wait_recv()
    for p in range(8):
        coarse[24 * p : 24 * p + 16, :] = vrecv[16 * p : 16 * p + 16, :]
        coarse[24 * p + 16 : 24 * p + 20, :] = vlo_r[p, 0:4, :]
        coarse[24 * p + 20 : 24 * p + 22, :] = vhi_r[p, 0:2, :]
    fine[...] = dot(coarse[...], t["spread"])

    def one_plane(p, carry):
        block = pl.ds(pl.multiple_of(24 * p, 8), 24)
        speed = dot(t["lift"], fine[block, :])
        x_speed, y_speed = speed[:24], speed[24:]
        values = jnp.concatenate([tile[block, :], side[block, :]], axis=1)
        for _ in range(2):
            values = advance(values, x_speed, y_speed)
        snew[p] = values[4:20, :128]
        return carry

    lax.fori_loop(0, 8, one_plane, 0)

    row8 = 8 * c + lax.broadcasted_iota(jnp.int32, (8, 128), 0)
    wave_x = jnp.where(row8 < 256, row8, row8 - 512)
    squared_x = jnp.square(wave_x.astype(jnp.float32) * (1.0 / 256.0))
    damping, keep = [], []
    for m in range(4):
        column = 128 * m + lax.broadcasted_iota(jnp.int32, (8, 128), 1)
        wave_y = jnp.where(column < 256, column, column - 512)
        squared_y = jnp.square(wave_y.astype(jnp.float32) * (1.0 / 256.0))
        damping.append(jnp.exp(-viscosity * time_step * (squared_x + squared_y)))
        keep.append(jnp.logical_and(3 * jnp.abs(wave_x) < 512, 3 * jnp.abs(wave_y) < 512))

    @pl.when(jnp.logical_not(kept))
    def _():
        for n in range(6):
            for m in range(4):
                lanes = slice(128 * m, 128 * m + 128)
                vnew[n, :, lanes] = damping[m] * vh[n, :, lanes]

    @pl.when(kept)
    def _():
        for d in range(1, 16):
            remote(send4.at[0], rows(recv4, 0, 16), s4.at[d], r4.at[d], plane_peers[d - 1]).wait_recv()
        gathered = [
            jnp.concatenate([recv4[pl.ds(4 * f + k, 16, stride=16), :] for k in range(4)], axis=0)
            for f in range(3)
        ]
        forcing = forward_y(t, gathered)
        for f in range(3):
            for ri in range(2):
                for m in range(4):
                    lanes = slice(128 * m, 128 * m + 128)
                    push = forcing[f][32 * ri + 8 * m : 32 * ri + 8 * m + 8]
                    n = 2 * f + ri
                    vnew[n, :, lanes] = damping[m] * (
                        vh[n, :, lanes] + time_step * jnp.where(keep[m], push, 0.0)
                    )

    for copy in sent1 + sentv + [
        edge_right, edge_left, rim_next, rim_prev, corner_next, corner_prev, far_up, far_down, near_up, near_down,
        pass_up, pass_down, far3, near_up3, near_down3,
    ] + sentr:
        copy.wait_send()
    for d in range(1, 16):
        to = (w + d) % 16

        @pl.when(jnp.logical_or(to < 6, to >= 10))
        def _():
            remote(send4.at[0], rows(recv4, 0, 16), s4.at[d], r4.at[d], plane_peers[d - 1]).wait_send()


def advance(values, x_speed, y_speed):
    height, breadth = values.shape

    def along(axis, step):
        return pltpu.roll(values, (-step) % values.shape[axis], axis)

    def parts(axis):
        two_back, back, ahead, two_ahead = (along(axis, s) for s in (-2, -1, 1, 2))
        grad = (two_back - two_ahead + 8.0 * (ahead - back)) * (1.0 / 12.0)
        lap = (16.0 * (ahead + back) - two_ahead - two_back - 30.0 * values) * (1.0 / 12.0)
        return grad, lap

    grad_x, lap_x = parts(1)
    grad_y, lap_y = parts(0)
    return values + substep * (diffusivity * (lap_x + lap_y) - (x_speed * grad_x + y_speed * grad_y))


def per_device(velocity_hat, scalar, tile_offset):
    consts = tables()
    f32 = jnp.float32
    vmem = pl.BlockSpec(memory_space=pltpu.VMEM)
    far = pl.BlockSpec(memory_space=pl.ANY)
    dma = pltpu.SemaphoreType.DMA

    def buf(*shape):
        return pltpu.VMEM(shape, f32)

    vnew, snew = pl.pallas_call(
        kernel,
        name="coupled_step",
        out_shape=(jax.ShapeDtypeStruct((6, 8, 512), f32), jax.ShapeDtypeStruct((8, 16, 128), f32)),
        in_specs=[far, far, pl.BlockSpec(memory_space=pltpu.SMEM)] + [far] * len(NAMES),
        out_specs=(vmem, vmem),
        scratch_shapes=[
            buf(384, 128), buf(384, 128), buf(4, 80, 128), buf(4, 80, 128), buf(2, 40, 128),
            buf(4, 40, 128), buf(160, 128), buf(12, 16, 128), buf(256, 128),
            buf(8, 16, 128), buf(128, 128), buf(8, 8, 128), buf(8, 8, 128), buf(8, 8, 128), buf(8, 8, 128),
            buf(2, 8, 128), buf(2, 8, 128), buf(2, 32, 128), buf(2, 32, 128), buf(8, 128), buf(2, 8, 128), buf(128, 128),
            buf(192, 128), buf(192, 128),
            buf(192, 128), buf(192, 256),
            dma((16,)), dma((16,)), dma((6,)), dma((6,)), dma((3,)), dma((3,)), dma((16,)), dma((16,)),
            dma((8,)), dma((8,)), dma((8,)), dma((8,)), dma((8,)), dma((8,)), dma((8,)), dma((8,)),
            pltpu.SemaphoreType.REGULAR, buf(6, 8, 512), buf(8, 16, 128), dma((2 + len(NAMES),)),
        ] + [buf(*consts[k].shape) for k in NAMES],
        compiler_params=pltpu.CompilerParams(collective_id=0, has_side_effects=True),
    )(velocity_hat.reshape(6, 8, 512), scalar, tile_offset, *[jnp.asarray(consts[k]) for k in NAMES])
    return vnew.reshape(3, 2, 1, 8, 512), snew


def solution(mesh):
    return jax.shard_map(
        per_device,
        mesh=mesh,
        in_specs=(P(None, None, ("group", "row"), "col", None), P("group", "col", "row"), P()),
        out_specs=(P(None, None, ("group", "row"), "col", None), P("group", "col", "row")),
        check_vma=False,
    )
```

```python
import math

import jax
import jax.numpy as jnp
import numpy as np
from jax import lax
from jax.experimental import pallas as pl
from jax.experimental.pallas import tpu as pltpu
from jax.sharding import PartitionSpec as P

time_step = 0.25
viscosity = 2.0
diffusivity = 0.15
substep = 0.2
MESH = pl.DeviceIdType.MESH

N, NC, NL = 512, 64, 8
KEPT = [0, 1, 2, 3, 4, 5, 10, 11, 12, 13, 14, 15]
ORDER = KEPT + [6, 7, 8, 9]


def tables():
    unit = 1.0 / math.sqrt(N)
    wave = np.arange(N)
    wave = np.where(wave < N // 2, wave, wave - N) / (N // 2)
    eye = np.eye(8)
    c_natural = np.arange(64)
    c_zw = np.array([4 * w + z for z in range(4) for w in range(16)])
    c_kept = np.array([4 * w + z for z in range(4) for w in ORDER])
    rows = np.arange(64)

    def angle(left, right, length):
        return 2 * np.pi * ((left[:, None] * right[None, :]) % length) / length

    eighth = np.arange(8)
    turn = np.exp(1j * angle(eighth, eighth, 8)) * unit

    first = []
    for e in range(2):
        part = np.zeros((2, 4, 8, 2, 2, 8, 8))
        for m in range(4):
            for l in range(8):
                v = turn[2 * m + e, l]
                for j in range(8):
                    part[0, m, j, 0, 0, l, j] = v.real
                    part[1, m, j, 0, 0, l, j] = -v.imag
                    part[0, m, j, 0, 1, l, j] = v.imag
                    part[1, m, j, 0, 1, l, j] = v.real
        part[:, :, :, 1, 0] = -part[:, :, :, 0, 1]
        part[:, :, :, 1, 1] = part[:, :, :, 0, 0]
        first.append(part.reshape(64, 256))

    lane = np.arange(128)
    twist_y = angle(rows, (lane // 8) % 8, N)
    twist_x = angle(rows, lane % 8, N)

    mixed = np.zeros((2, 2, 8, 8, 2, 8, 8))
    forward = np.zeros((2, 8, 8, 2, 2, 8, 8))
    last = [np.zeros((2, 2, 8, 8, 2, 4, 8)) for _ in range(2)]
    for l in range(8):
        for j in range(8):
            for p in range(8):
                v = turn[j, p]
                for half in range(2):
                    mixed[0, 0, l, j, half, p, l] = v.real
                    mixed[0, 1, l, j, half, p, l] = -v.imag
                    mixed[1, 0, l, j, half, p, l] = -v.imag
                    mixed[1, 1, l, j, half, p, l] = -v.real
                forward[0, p, l, 0, 0, l, j] = v.real
                forward[0, p, l, 0, 1, l, j] = -v.imag
                forward[0, p, l, 1, 0, l, j] = v.imag
                forward[0, p, l, 1, 1, l, j] = v.real
            for m in range(4):
                for e in range(2):
                    v = turn[2 * m + e, l]
                    t = last[e]
                    t[0, 0, l, j, 0, m, j] = v.real
                    t[1, 1, l, j, 0, m, j] = v.real
                    t[0, 1, l, j, 0, m, j] = v.imag
                    t[1, 0, l, j, 0, m, j] = -v.imag
                    t[0, 1, l, j, 1, m, j] = v.real
                    t[1, 0, l, j, 1, m, j] = -v.real
                    t[0, 0, l, j, 1, m, j] = -v.imag
                    t[1, 1, l, j, 1, m, j] = -v.imag
    forward_y = np.zeros_like(forward)
    forward_y[1] = forward[0]

    def pair(order):
        t = angle(order, rows, 64)
        return np.concatenate([np.cos(t), np.sin(t)], axis=1)

    stacked = angle(rows, c_zw, 64)
    kappa_y = np.zeros((2, 64, 2, 4, 8))
    for e in range(2):
        for m in range(4):
            kappa_y[e, :, :, m, :] = wave[64 * (2 * m + e) + rows][:, None, None]
    kappa_x = wave[8 * c_zw[:, None] + (lane % 8)[None, :]]

    spread = np.zeros((128, 256))
    for f in range(-2, 130):
        k = f // 2 + 1
        if f % 2 == 0:
            spread[k, f % 256] = 1.0
        else:
            spread[k, f % 256] = 0.5
            spread[k + 1, f % 256] = 0.5
    lift = np.zeros((2, 24, 24))
    for v in range(2):
        def slot(row):
            if row < 0:
                return 20 + v
            return 8 * v + row if row < 8 else 16 + 2 * v + row - 8
        for f in range(-2, 18):
            k = f // 2
            if f % 2 == 0:
                lift[v, f + 4, slot(k)] = 1.0
            else:
                lift[v, f + 4, slot(k)] = 0.5
                lift[v, f + 4, slot(k + 1)] = 0.5

    out = dict(
        first0=first[0], first1=first[1],
        tyc=np.cos(twist_y), tys=np.sin(twist_y), txc=np.cos(twist_x), txs=np.sin(twist_x),
        cs1=pair(c_natural), cs3=np.concatenate([np.cos(stacked).T, np.sin(stacked).T]).reshape(2, 64, 64).transpose(0, 1, 2).reshape(128, 64),
        mixed=mixed.reshape(256, 128), fx=forward.reshape(128, 256), fy=forward_y.reshape(128, 256),
        cs4=pair(c_kept), last0=last[0].reshape(256, 64), last1=last[1].reshape(256, 64),
        ky=kappa_y.reshape(128, 64), kx=kappa_x, spread=spread, lift=lift.reshape(48, 24),
    )
    flat = angle(rows, c_zw, 64)
    out["cs3"] = np.concatenate([np.cos(flat), np.sin(flat)], axis=0)
    return {k: np.asarray(v, np.float32) for k, v in out.items()}


NAMES = ["first0", "first1", "tyc", "tys", "txc", "txs", "cs1", "cs3", "mixed", "fx", "fy", "cs4",
         "last0", "last1", "ky", "kx", "spread", "lift"]


def split(a):
    high = a.astype(jnp.bfloat16)
    return high, (a - high.astype(jnp.float32)).astype(jnp.bfloat16)


def dot(a, b):
    (a_high, a_low), (b_high, b_low) = split(a), split(b)

    def product(x, y):
        return jnp.dot(x, y, preferred_element_type=jnp.float32)

    return product(a_high, b_high) + (product(a_high, b_low) + product(a_low, b_high))


def inverse_y(t, spectra, kappa_x):
    turned = []
    for comp in range(3):
        stacked = jnp.concatenate(
            [spectra(comp, ri)[:, 128 * m : 128 * m + 128] for ri in range(2) for m in range(4)], axis=0
        )
        turned.append(stacked.T)
    spin_x = turned[2] * t["ky"]
    spin_z = turned[1] * kappa_x - turned[0] * t["ky"]
    fields = turned + [spin_x, spin_z]
    even = jnp.concatenate([f[:64] for f in fields], axis=0)
    odd = jnp.concatenate([f[64:] for f in fields], axis=0)
    mixed = dot(even, t["first0"]) + dot(odd, t["first1"])
    upper, lower = [], []
    for n in range(5):
        plain = mixed[64 * n : 64 * n + 64, :128]
        times_i = mixed[64 * n : 64 * n + 64, 128:]
        if n >= 3:
            plain, times_i = times_i, -plain
        upper.append(plain * t["tyc"] + times_i * t["tys"])
        lower.append(times_i * t["tyc"] - plain * t["tys"])
    both = jnp.concatenate([jnp.concatenate(upper, axis=1), jnp.concatenate(lower, axis=1)], axis=0)
    blocks = dot(t["cs1"], both)
    return [blocks[:, 128 * n : 128 * n + 128] for n in range(5)]


def inverse_x(t, blocks):
    u, v, w, spin_x, spin_z = blocks
    six = [u, v, w, spin_x, w * t["kx"], spin_z]
    summed = dot(t["cs3"], jnp.concatenate(six, axis=1))
    rows = []
    for n in range(6):
        first = summed[:64, 128 * n : 128 * n + 128]
        second = summed[64:, 128 * n : 128 * n + 128]
        a = first * t["txc"] - second * t["txs"]
        b = first * t["txs"] + second * t["txc"]
        if n == 4:
            a, b = b, -a
        rows.append(jnp.concatenate([a, b], axis=1))
    fields = dot(jnp.concatenate(rows, axis=0), t["mixed"])
    return [fields[64 * n : 64 * n + 64] for n in range(6)]


def forward_x(t, fields):
    u, v, w, ox, oy, oz = fields
    left = lax.broadcasted_iota(jnp.int32, (64, 128), 1) < 64
    product_xy = jnp.where(left, v, w) * jnp.where(left, oz, ox) - jnp.where(left, w, u) * jnp.where(left, oy, oz)
    product_z = u * oy - v * ox
    mixed = [dot(product_xy, t["fx"]), dot(product_xy, t["fy"]), dot(product_z, t["fx"])]
    upper, lower = [], []
    for m in mixed:
        plain, times_i = m[:, :128], m[:, 128:]
        upper.append(plain * t["txc"] - times_i * t["txs"])
        lower.append(-(times_i * t["txc"] + plain * t["txs"]))
    both = jnp.concatenate([jnp.concatenate(upper, axis=1), jnp.concatenate(lower, axis=1)], axis=0)
    blocks = dot(t["cs4"], both)
    return [blocks[:, 128 * n : 128 * n + 128] for n in range(3)]


def forward_y(t, blocks):
    summed = dot(t["cs3"], jnp.concatenate(blocks, axis=1))
    rows = []
    for n in range(3):
        first = summed[:64, 128 * n : 128 * n + 128]
        second = summed[64:, 128 * n : 128 * n + 128]
        rows.append(
            jnp.concatenate(
                [first * t["tyc"] - second * t["tys"], first * t["tys"] + second * t["tyc"]], axis=1
            )
        )
    rows = jnp.concatenate(rows, axis=0)
    even, odd = dot(rows, t["last0"]), dot(rows, t["last1"])
    return [
        jnp.concatenate([even[64 * n : 64 * n + 64], odd[64 * n : 64 * n + 64]], axis=0).T for n in range(3)
    ]


def kernel(vh_far, sc_far, off, *rest):
    n_tables = len(NAMES)
    far_tables, near_tables = rest[:n_tables], rest[-n_tables:]
    rest = rest[:-n_tables]
    (push_out, snew, send1, recv1, send2, recv2, relay2, send3, recv3, send4, recv4,
     vsend, vrecv, vlo_s, vhi_s, vlo_r, vhi_r, edge_s, edge_r, rim_s, rim_r, corner_s, corner_r, turned, tile, side, coarse, fine,
     s1, r1, s2, r2, s3, r3, s4, r4, sv, rv, sl, rl, sh, rh, sm, rm, row_sem, vh, sc, load) = rest[n_tables:]

    g = lax.axis_index("group")
    r = lax.axis_index("row")
    c = lax.axis_index("col")
    w, z = c // 4, c % 4
    z_up, z_down, z_far = (z + 1) % 4, (z + 3) % 4, (z + 2) % 4
    up, down, opposite = (g, r, 4 * w + z_up), (g, r, 4 * w + z_down), (g, r, 4 * w + z_far)
    c_next, c_prev = (g, r, (c + 1) % 64), (g, r, (c + 63) % 64)
    r_next, r_prev = (g, (r + 1) % 8, c), (g, (r + 7) % 8, c)
    plane_peers = [(g, r, 4 * ((w + d) % 16) + z) for d in range(1, 16)]
    row_peers = [(g, (r + d) % 8, c) for d in range(1, 8)]
    kept = jnp.logical_or(w < 6, w >= 10)

    barrier = pltpu.get_barrier_semaphore()
    greeted = plane_peers + row_peers + [up, down, c_next, c_prev]
    for peer in greeted:
        pl.semaphore_signal(barrier, inc=1, device_id=peer, device_id_type=MESH)

    fetched = [pltpu.make_async_copy(vh_far, vh, load.at[0]), pltpu.make_async_copy(sc_far, sc, load.at[1])]
    for n in range(n_tables):
        fetched.append(pltpu.make_async_copy(far_tables[n], near_tables[n], load.at[2 + n]))
    for copy in fetched:
        copy.start()
    for copy in fetched:
        copy.wait()
    t = {name: near_tables[n][...] for n, name in enumerate(NAMES)}

    def remote(src, dst, ssem, rsem, peer):
        return pltpu.make_async_remote_copy(
            src_ref=src, dst_ref=dst, send_sem=ssem, recv_sem=rsem, device_id=peer, device_id_type=MESH
        )

    def rows(ref, start, size):
        return ref.at[pl.ds(pl.multiple_of(start, 8), size), :]

    lane64 = lax.broadcasted_iota(jnp.int32, (1, 64), 1)
    wave = 8 * c + lane64 % 8
    kappa = jnp.where(wave < 256, wave, wave - 512).astype(jnp.float32) * (1.0 / 256.0)
    blocks = inverse_y(t, lambda comp, ri: vh[2 * comp + ri], kappa)
    zero = jnp.zeros((4, 128), jnp.float32)
    for d in range(16):
        part = [b[4 * d : 4 * d + 4] for b in blocks] + [zero]
        send1[24 * d : 24 * d + 24, :] = jnp.concatenate(part, axis=0)

    side[...] = jnp.zeros_like(side)
    coarse[...] = jnp.zeros_like(coarse)
    for p in range(8):
        turned[16 * p : 16 * p + 16, :] = sc[p]
        tile[24 * p + 4 : 24 * p + 20, :] = sc[p]
    flat = turned[...].T
    edge_s[0] = flat[120:128]
    edge_s[1] = flat[0:8]
    for i in range(4):
        rim_s[0, 8 * i : 8 * i + 8, :] = turned[pl.ds(12 + i, 8, stride=16), :]
        rim_s[1, 8 * i : 8 * i + 8, :] = turned[pl.ds(i, 8, stride=16), :]

    pl.semaphore_wait(barrier, len(greeted))
    for peer in row_peers:
        pl.semaphore_signal(row_sem, inc=1, device_id=peer, device_id_type=MESH)

    edge_right = remote(edge_s.at[0], edge_r.at[0], sm.at[0], rm.at[0], r_next)
    edge_left = remote(edge_s.at[1], edge_r.at[1], sm.at[1], rm.at[1], r_prev)
    rim_next = remote(rim_s.at[0], rim_r.at[0], sm.at[2], rm.at[2], c_next)
    rim_prev = remote(rim_s.at[1], rim_r.at[1], sm.at[3], rm.at[3], c_prev)
    edge_right.start()
    edge_left.start()
    sent1 = []
    for d in range(1, 16):
        to = (w + d) % 16
        copy = remote(rows(send1, 24 * to, 20), rows(recv1, 24 * w, 20), s1.at[d], r1.at[d], plane_peers[d - 1])
        copy.start()
        sent1.append(copy)
    rim_next.start()
    rim_prev.start()
    mine = pl.ds(pl.multiple_of(24 * w, 8), 24)
    recv1[mine, :] = send1[mine, :]
    for copy in sent1:
        copy.wait_recv()
    for k in range(4):
        for f in range(5):
            send2[k, 16 * f : 16 * f + 16, :] = recv1[pl.ds(4 * f + k, 16, stride=24), :]

    half = 40
    far_up = remote(send2.at[z_far, pl.ds(0, half)], relay2.at[0], s2.at[0], r2.at[0], up)
    far_down = remote(send2.at[z_far, pl.ds(half, half)], relay2.at[1], s2.at[1], r2.at[1], down)
    near_up = remote(send2.at[z_up], recv2.at[z], s2.at[2], r2.at[2], up)
    near_down = remote(send2.at[z_down], recv2.at[z], s2.at[3], r2.at[3], down)
    far_up.start()
    far_down.start()
    near_up.start()
    near_down.start()
    recv2[z] = send2[z]
    far_up.wait_recv()
    pass_up = remote(relay2.at[0], recv2.at[z_down, pl.ds(0, half)], s2.at[4], r2.at[4], up)
    pass_up.start()
    far_down.wait_recv()
    pass_down = remote(relay2.at[1], recv2.at[z_up, pl.ds(half, half)], s2.at[5], r2.at[5], down)
    pass_down.start()

    edge_right.wait_recv()
    edge_left.wait_recv()
    corner_s[...] = jnp.concatenate(
        [edge_r[1, 0:2, :], edge_r[0, 6:8, :], jnp.zeros((4, 128), jnp.float32)], axis=0
    )
    corner_next = remote(corner_s, corner_r.at[0], sm.at[6], rm.at[6], c_next)
    corner_prev = remote(corner_s, corner_r.at[1], sm.at[7], rm.at[7], c_prev)
    corner_next.start()
    corner_prev.start()
    beside = jnp.concatenate([edge_r[1], jnp.zeros((112, 128), jnp.float32), edge_r[0]], axis=0).T
    for p in range(8):
        side[24 * p + 4 : 24 * p + 20, :] = beside[16 * p : 16 * p + 16]

    near_up.wait_recv()
    near_down.wait_recv()
    pass_up.wait_recv()
    pass_down.wait_recv()

    landed = [
        jnp.concatenate([recv2[k, 16 * f : 16 * f + 16, :] for k in range(4)], axis=0) for f in range(5)
    ]
    fields = inverse_x(t, landed)
    leaving = forward_x(t, fields)
    for k in range(4):
        for f in range(3):
            send3[k, 12 * f : 12 * f + 12, :] = leaving[f][16 * k : 16 * k + 12]
        send3[k, 36:40, :] = zero
    kept_rows = pl.ds(0, 36)
    far3 = remote(send3.at[z_far, kept_rows], rows(recv3, 40 * z, 36), s3.at[0], r3.at[0], opposite)
    near_up3 = remote(send3.at[z_up, kept_rows], rows(recv3, 40 * z, 36), s3.at[1], r3.at[1], up)
    near_down3 = remote(send3.at[z_down, kept_rows], rows(recv3, 40 * z, 36), s3.at[2], r3.at[2], down)

    @pl.when(z % 2 == 0)
    def _():
        far3.start()

    near_up3.start()
    near_down3.start()

    @pl.when(z % 2 == 1)
    def _():
        far3.start()

    recv3[pl.ds(pl.multiple_of(40 * z, 8), 40), :] = send3[z]

    left = lax.broadcasted_iota(jnp.int32, (64, 128), 1) < 64
    speeds = jnp.where(left, fields[0], fields[1]).T
    lines = []
    for f in range(2):
        lines.append(
            jnp.concatenate([speeds[64 * f + 8 * p : 64 * f + 8 * p + 8, :] for p in range(8)], axis=1)
        )
    lines = jnp.concatenate(lines, axis=0)
    rolled = pltpu.roll(lines, (513 - off[0]) % 512, 1)
    shifted = pltpu.roll(rolled, 448, 1)
    for k in range(4):
        vsend[2 * k] = rolled[:, 128 * k : 128 * k + 128]
        vsend[2 * k + 1] = shifted[:, 128 * k : 128 * k + 128]
        for n, source in enumerate((rolled, shifted)):
            part = source[:, 128 * k : 128 * k + 128]
            vlo_s[2 * k + n] = jnp.concatenate([part[0:2], part[8:10], zero], axis=0)
            vhi_s[2 * k + n] = jnp.concatenate([part[7:8], part[15:16], zero, zero[:2]], axis=0)
    pl.semaphore_wait(row_sem, 7)
    sentv = []
    for d in range(1, 8):
        copy = remote(vsend.at[(r + d) % 8], rows(vrecv, 16 * r, 16), sv.at[d], rv.at[d], row_peers[d - 1])
        copy.start()
        sentv.append(copy)
    sentr = []
    for d in range(8):
        to = (r + d) % 8
        low = remote(vlo_s.at[to, pl.ds(0, 4)], vlo_r.at[r, pl.ds(0, 4)], sl.at[d], rl.at[d], (g, to, (c + 63) % 64))
        high = remote(vhi_s.at[to, pl.ds(0, 2)], vhi_r.at[r, pl.ds(0, 2)], sh.at[d], rh.at[d], (g, to, (c + 1) % 64))
        low.start()
        high.start()
        sentr += [low, high]
    vrecv[pl.ds(pl.multiple_of(16 * r, 8), 16), :] = vsend[r]

    near_up3.wait_recv()
    near_down3.wait_recv()
    far3.wait_recv()

    for k in range(12):
        part = [recv3[pl.ds(12 * f + k, 4, stride=40), :] for f in range(3)] + [zero]
        send4[k] = jnp.concatenate(part, axis=0)
    for d in range(1, 16):
        to = (w + d) % 16
        slot = jnp.where(to < 6, to, to - 4)

        @pl.when(jnp.logical_or(to < 6, to >= 10))
        def _():
            remote(send4.at[slot, pl.ds(0, 12)], rows(recv4, 16 * w, 12), s4.at[d], r4.at[d], plane_peers[d - 1]).start()

    @pl.when(kept)
    def _():
        recv4[pl.ds(pl.multiple_of(16 * w, 8), 16), :] = send4[jnp.where(w < 6, w, w - 4)]

    rim_next.wait_recv()
    rim_prev.wait_recv()
    for i in range(4):
        tile[pl.ds(i, 8, stride=24), :] = rim_r[0, 8 * i : 8 * i + 8, :]
        tile[pl.ds(20 + i, 8, stride=24), :] = rim_r[1, 8 * i : 8 * i + 8, :]
    corner_next.wait_recv()
    corner_prev.wait_recv()
    for n in range(2):
        turned[...] = jnp.concatenate(
            [corner_r[n, 0:2, :], jnp.zeros((124, 128), jnp.float32), corner_r[n, 2:4, :]], axis=0
        ).T
        for i in range(2):
            side[pl.ds(2 + 18 * n + i, 8, stride=24), :] = turned[pl.ds(14 * (1 - n) + i, 8, stride=16), :]
    for copy in sentv + sentr:
        copy.wait_recv()
    for p in range(8):
        coarse[24 * p : 24 * p + 16, :] = vrecv[16 * p : 16 * p + 16, :]
        coarse[24 * p + 16 : 24 * p + 20, :] = vlo_r[p, 0:4, :]
        coarse[24 * p + 20 : 24 * p + 22, :] = vhi_r[p, 0:2, :]
    fine[...] = dot(coarse[...], t["spread"])

    def one_plane(p, carry):
        block = pl.ds(pl.multiple_of(24 * p, 8), 24)
        speed = dot(t["lift"], fine[block, :])
        x_speed, y_speed = speed[:24], speed[24:]
        values = jnp.concatenate([tile[block, :], side[block, :]], axis=1)
        for _ in range(2):
            values = advance(values, x_speed, y_speed)
        snew[p] = values[4:20, :128]
        return carry

    lax.fori_loop(0, 8, one_plane, 0)

    row8 = 8 * c + lax.broadcasted_iota(jnp.int32, (8, 128), 0)
    wave_x = jnp.where(row8 < 256, row8, row8 - 512)
    keep = []
    for m in range(4):
        column = 128 * m + lax.broadcasted_iota(jnp.int32, (8, 128), 1)
        wave_y = jnp.where(column < 256, column, column - 512)
        keep.append(jnp.logical_and(3 * jnp.abs(wave_x) < 512, 3 * jnp.abs(wave_y) < 512))

    @pl.when(jnp.logical_not(kept))
    def _():
        push_out[...] = jnp.zeros_like(push_out)

    @pl.when(kept)
    def _():
        for d in range(1, 16):
            remote(send4.at[0, pl.ds(0, 12)], rows(recv4, 0, 12), s4.at[d], r4.at[d], plane_peers[d - 1]).wait_recv()
        gathered = [
            jnp.concatenate([recv4[pl.ds(4 * f + k, 16, stride=16), :] for k in range(4)], axis=0)
            for f in range(3)
        ]
        forcing = forward_y(t, gathered)
        for f in range(3):
            for ri in range(2):
                for m in range(4):
                    lanes = slice(128 * m, 128 * m + 128)
                    push = forcing[f][32 * ri + 8 * m : 32 * ri + 8 * m + 8]
                    n = 2 * f + ri
                    push_out[n, :, lanes] = time_step * jnp.where(keep[m], push, 0.0)

    for copy in sent1 + sentv + [
        edge_right, edge_left, rim_next, rim_prev, corner_next, corner_prev, far_up, far_down, near_up, near_down,
        pass_up, pass_down, far3, near_up3, near_down3,
    ] + sentr:
        copy.wait_send()
    for d in range(1, 16):
        to = (w + d) % 16

        @pl.when(jnp.logical_or(to < 6, to >= 10))
        def _():
            remote(send4.at[0, pl.ds(0, 12)], rows(recv4, 0, 12), s4.at[d], r4.at[d], plane_peers[d - 1]).wait_send()


def advance(values, x_speed, y_speed):
    height, breadth = values.shape

    def along(axis, step):
        return pltpu.roll(values, (-step) % values.shape[axis], axis)

    def parts(axis):
        two_back, back, ahead, two_ahead = (along(axis, s) for s in (-2, -1, 1, 2))
        grad = (two_back - two_ahead + 8.0 * (ahead - back)) * (1.0 / 12.0)
        lap = (16.0 * (ahead + back) - two_ahead - two_back - 30.0 * values) * (1.0 / 12.0)
        return grad, lap

    grad_x, lap_x = parts(1)
    grad_y, lap_y = parts(0)
    return values + substep * (diffusivity * (lap_x + lap_y) - (x_speed * grad_x + y_speed * grad_y))


def per_device(velocity_hat, scalar, tile_offset):
    consts = tables()
    f32 = jnp.float32
    vmem = pl.BlockSpec(memory_space=pltpu.VMEM)
    far = pl.BlockSpec(memory_space=pl.ANY)
    dma = pltpu.SemaphoreType.DMA

    def buf(*shape):
        return pltpu.VMEM(shape, f32)

    push, snew = pl.pallas_call(
        kernel,
        name="coupled_step",
        out_shape=(jax.ShapeDtypeStruct((6, 8, 512), f32), jax.ShapeDtypeStruct((8, 16, 128), f32)),
        in_specs=[far, far, pl.BlockSpec(memory_space=pltpu.SMEM)] + [far] * len(NAMES),
        out_specs=(vmem, vmem),
        scratch_shapes=[
            buf(384, 128), buf(384, 128), buf(4, 80, 128), buf(4, 80, 128), buf(2, 40, 128),
            buf(4, 40, 128), buf(160, 128), buf(12, 16, 128), buf(256, 128),
            buf(8, 16, 128), buf(128, 128), buf(8, 8, 128), buf(8, 8, 128), buf(8, 8, 128), buf(8, 8, 128),
            buf(2, 8, 128), buf(2, 8, 128), buf(2, 32, 128), buf(2, 32, 128), buf(8, 128), buf(2, 8, 128), buf(128, 128),
            buf(192, 128), buf(192, 128),
            buf(192, 128), buf(192, 256),
            dma((16,)), dma((16,)), dma((6,)), dma((6,)), dma((3,)), dma((3,)), dma((16,)), dma((16,)),
            dma((8,)), dma((8,)), dma((8,)), dma((8,)), dma((8,)), dma((8,)), dma((8,)), dma((8,)),
            pltpu.SemaphoreType.REGULAR, buf(6, 8, 512), buf(8, 16, 128), dma((2 + len(NAMES),)),
        ] + [buf(*consts[k].shape) for k in NAMES],
        compiler_params=pltpu.CompilerParams(collective_id=0, has_side_effects=True),
    )(velocity_hat.reshape(6, 8, 512), scalar, tile_offset, *[jnp.asarray(consts[k]) for k in NAMES])
    row = 8 * lax.axis_index("col") + jnp.arange(8, dtype=jnp.int32)
    column = jnp.arange(N, dtype=jnp.int32)

    def squared(index):
        return jnp.square(jnp.where(index < N // 2, index, index - N).astype(f32) / (N // 2))

    damping = jnp.exp(-viscosity * time_step * (squared(row)[:, None] + squared(column)[None, :]))
    return damping * (velocity_hat + push.reshape(velocity_hat.shape)), snew


def solution(mesh):
    return jax.shard_map(
        per_device,
        mesh=mesh,
        in_specs=(P(None, None, ("group", "row"), "col", None), P("group", "col", "row"), P()),
        out_specs=(P(None, None, ("group", "row"), "col", None), P("group", "col", "row")),
        check_vma=False,
    )
```
